32 devices in a mesh: batch: 1 (over z), w: 4 (over y), h: 8 (over x, core).
Axes of the slice: x: 4, y: 4, z: 1, core: 2. Of those that a mesh axis runs over, the one named last changes fastest.
The devices are a block of a 4x4x8 slice.
Arguments:
- image: bfloat16 [512, 128, 256, 4], P('batch', 'h', 'w')
- down_w1: bfloat16 [3, 3, 4, 32], replicated
- down_v1: float32 [3, 32], replicated
- refine_w1: bfloat16 [3, 3, 32, 32], replicated
- refine_v1: float32 [3, 32], replicated
- down_w2: bfloat16 [3, 3, 32, 64], replicated
- down_v2: float32 [3, 64], replicated
- refine_w2: bfloat16 [3, 3, 64, 64], replicated
- refine_v2: float32 [3, 64], replicated
- down_w3: bfloat16 [3, 3, 64, 128], replicated
- down_v3: float32 [3, 128], replicated
- refine_w3: bfloat16 [3, 3, 128, 128], replicated
- refine_v3: float32 [3, 128], replicated
Outputs:
- output: bfloat16 [512, 16, 32, 128], P('batch', 'h', 'w')
All inputs are finite; a program needn't handle non-finite values.
Results may differ from the reference program's by a relative error of at most 0.00349926.
Values are sent between devices in bfloat16 or wider.
A program may use at most 768 MiB of HBM per device.

```python
import jax
import jax.numpy as jnp
from jax import lax

IMAGES = 512
IMG_HEIGHT = 128
IMG_WIDTH = 256
CHAN_IN = 4
CHAN_ONE = 32
GROUPS = 8
NORM_EPS = 1e-5


def draw_affine(key, channels):
    bias_key, scale_key, shift_key = jax.random.split(key, 3)
    bias = 0.5 * jax.random.normal(bias_key, (channels,), jnp.float32)
    scale = 1.0 + 0.3 * jax.random.normal(scale_key, (channels,), jnp.float32)
    shift = 0.3 * jax.random.normal(shift_key, (channels,), jnp.float32)
    return jnp.stack([bias, scale, shift])


def setup_inputs(seed: int = 0, part: int = 0) -> dict:
    shared_key, image_root = jax.random.split(jax.random.key(seed))
    image_key = jax.random.fold_in(image_root, part)
    noise_key, slope_key, level_key = jax.random.split(image_key, 3)
    noise = jax.random.normal(noise_key, (IMAGES, IMG_HEIGHT, IMG_WIDTH, CHAN_IN), jnp.float32)
    slopes = jax.random.normal(slope_key, (2, IMAGES, 1, 1, CHAN_IN), jnp.float32)
    levels = 0.5 * jax.random.normal(level_key, (IMAGES, 1, 1, CHAN_IN), jnp.float32)
    row_pos = (jnp.arange(IMG_HEIGHT, dtype=jnp.float32) + 0.5) * (2.0 / IMG_HEIGHT) - 1.0
    col_pos = (jnp.arange(IMG_WIDTH, dtype=jnp.float32) + 0.5) * (2.0 / IMG_WIDTH) - 1.0
    ramp = slopes[0] * row_pos[:, None, None] + slopes[1] * col_pos[:, None]
    image = (noise + 1.5 * ramp + levels).astype(jnp.bfloat16)
    widths = [CHAN_IN, CHAN_ONE, 2 * CHAN_ONE, 4 * CHAN_ONE]
    weight_keys = jax.random.split(shared_key, 12)
    inputs = {"image": image}
    for stage in range(3):
        chan_prev = widths[stage]
        chan_next = widths[stage + 1]
        down_w = jax.random.normal(weight_keys[4 * stage], (3, 3, chan_prev, chan_next), jnp.float32) * (9 * chan_prev) ** -0.5
        refine_w = jax.random.normal(weight_keys[4 * stage + 2], (3, 3, chan_next, chan_next), jnp.float32) * (9 * chan_next) ** -0.5
        inputs["down_w" + str(stage + 1)] = down_w.astype(jnp.bfloat16)
        inputs["down_v" + str(stage + 1)] = draw_affine(weight_keys[4 * stage + 1], chan_next)
        inputs["refine_w" + str(stage + 1)] = refine_w.astype(jnp.bfloat16)
        inputs["refine_v" + str(stage + 1)] = draw_affine(weight_keys[4 * stage + 3], chan_next)
    return inputs


def conv_norm(inputs, kernel, affine, stride):
    summed = lax.conv_general_dilated(inputs.astype(jnp.float32), kernel.astype(jnp.float32), (stride, stride), ((1, 1), (1, 1)), dimension_numbers=("NHWC", "HWIO", "NHWC")) + affine[0]
    out_shape = summed.shape
    grouped = summed.reshape(out_shape[0], out_shape[1], out_shape[2], GROUPS, out_shape[3] // GROUPS)
    grp_mean = jnp.mean(grouped, axis=(1, 2, 4), keepdims=True)
    centered = grouped - grp_mean
    grp_var = jnp.mean(jnp.square(centered), axis=(1, 2, 4), keepdims=True)
    normed = (centered * lax.rsqrt(grp_var + NORM_EPS)).reshape(out_shape)
    return jax.nn.relu(normed * affine[1] + affine[2]).astype(jnp.bfloat16)


def reference(image, down_w1, down_v1, refine_w1, refine_v1, down_w2, down_v2, refine_w2, refine_v2, down_w3, down_v3, refine_w3, refine_v3):
    stages = ((down_w1, down_v1, refine_w1, refine_v1), (down_w2, down_v2, refine_w2, refine_v2), (down_w3, down_v3, refine_w3, refine_v3))

    def one_image(single):
        current = single[None]
        for down_w, down_v, refine_w, refine_v in stages:
            current = conv_norm(current, down_w, down_v, 2)
            current = conv_norm(current, refine_w, refine_v, 1)
        return current[0]

    return lax.map(one_image, image)
```

```python
import functools

import jax
import jax.numpy as jnp
from jax import lax
from jax.experimental import pallas as pl
from jax.experimental.pallas import tpu as pltpu
from jax.sharding import PartitionSpec as P

NORM_GROUPS = 8
NORM_EPS = 1e-5
CHUNKS = 2
BLOCKS = ((2, 1, 8), (1, 2, 4), (2, 1, 2), (1, 2, 2), (2, 1, 2), (1, 1, 2))


def patch_shape(stride, bh, bw, first):
    rows = (bh - 1) * stride + 3
    cols = (bw - 1) * stride + 3
    if first:
        cols = bw * stride + 4
    return rows, cols


def block_weights(kernel, stride, bh, bw, first):
    rows, cols = patch_shape(stride, bh, bw, first)
    off = 3 if first else 0
    flipped = kernel.transpose(3, 0, 1, 2)
    parts = []
    for i in range(bh):
        for j in range(bw):
            top, left = stride * i, off + stride * j
            padded = jnp.pad(flipped, ((0, 0), (top, rows - 3 - top), (left, cols - 3 - left), (0, 0)))
            parts.append(padded.reshape(kernel.shape[3], -1))
    return jnp.concatenate(parts, axis=0)


def encoder_kernel(cfg, x_ref, *refs):
    th, tw, c0, widths, grid_h, grid_w, imgs = cfg
    tiles = grid_h * grid_w
    lanes = tiles * imgs
    w_refs, v_refs = refs[0:6], refs[6:12]
    out_ref = refs[12]
    xp, acc_a, y1, z1, y2, z2, y3, s_ref = refs[13:]

    def iota(shape, dim):
        return lax.broadcasted_iota(jnp.int32, shape, dim)

    src = iota((lanes, lanes), 0)
    dst = iota((lanes, lanes), 1)

    def perm(dh, dw):
        t = dst // imgs
        h, w = t % grid_h + dh, t // grid_h + dw
        inside = (h >= 0) & (h < grid_h) & (w >= 0) & (w < grid_w)
        want = (w * grid_h + h) * imgs + dst % imgs
        return jnp.where(inside & (src == want), 1.0, 0.0).astype(jnp.bfloat16)

    above, below, left, right = perm(-1, 0), perm(1, 0), perm(0, -1), perm(0, 1)
    same_image = jnp.where(src % imgs == dst % imgs, 1.0, 0.0)

    def move(value, matrix):
        return jnp.dot(value, matrix, preferred_element_type=jnp.float32).astype(jnp.bfloat16)

    def halos(buf, rows, cols, unit, both):
        buf[0] = move(buf[rows], above)
        if both:
            buf[rows + 1] = move(buf[1], below)
        for r in range(rows + (2 if both else 1)):
            buf[r, 0:unit] = move(buf[r, cols * unit:(cols + 1) * unit], left)
            if both:
                buf[r, (cols + 1) * unit:(cols + 2) * unit] = move(buf[r, unit:2 * unit], right)

    def conv(buf, w_ref, stride, bh, bw, ci, co, out_h, out_w, first):
        rows, cols = patch_shape(stride, bh, bw, first)
        s_ref[:, 0:co] = jnp.zeros((2, co, lanes), jnp.float32)

        def row_body(i, carry):
            for j in range(out_w // bw):
                start = j * bw * stride * ci
                patch = jnp.concatenate([buf[i * (bh * stride) + r, start:start + cols * ci] for r in range(rows)], axis=0)
                res = jnp.dot(w_ref[...], patch, preferred_element_type=jnp.float32)
                parts = [res[p * co:(p + 1) * co] for p in range(bh * bw)]
                s_ref[0, 0:co] += functools.reduce(jnp.add, parts)
                s_ref[1, 0:co] += functools.reduce(jnp.add, [p * p for p in parts])
                for b in range(bh):
                    acc_a[i * bh + b, j * bw * co:(j + 1) * bw * co] = res[b * bw * co:(b + 1) * bw * co]
            return carry

        lax.fori_loop(0, out_h // bh, row_body, 0)

    def stats(v_ref, co, pixels):
        per = co // NORM_GROUPS
        group = jnp.where(iota((co, co), 0) // per == iota((co, co), 1) // per, 1.0, 0.0)
        hi = lax.Precision.HIGHEST
        tot = jnp.dot(s_ref[:, 0:co].reshape(2 * co, lanes), same_image, precision=hi, preferred_element_type=jnp.float32) / pixels
        mean_c, sq_c = tot[0:co], tot[co:2 * co]
        var_c = jnp.maximum(sq_c - mean_c * mean_c, 0.0)
        bias, gain, shift = v_ref[:, 0:1], v_ref[:, 1:2], v_ref[:, 2:3]
        mean_a = mean_c + bias
        m = jnp.dot(group, mean_a, precision=hi, preferred_element_type=jnp.float32) / per
        dev = mean_a - m
        q = jnp.dot(group, var_c + dev * dev, precision=hi, preferred_element_type=jnp.float32) / per
        scale = lax.rsqrt(q + NORM_EPS) * gain
        return scale, shift + (bias - m) * scale

    def normalise(scale, offset, co, out_h, out_w, dst_buf):
        def row_body(i, carry):
            for j in range(out_w):
                val = acc_a[i, j * co:(j + 1) * co]
                dst_buf[i + 1, (j + 1) * co:(j + 2) * co] = jnp.maximum(val * scale + offset, 0.0).astype(jnp.bfloat16)
            return carry

        lax.fori_loop(0, out_h, row_body, 0)

    width0 = tw * c0
    unit0 = 4 * c0

    def load_body(r, carry):
        block = x_ref[:, pl.ds(pl.multiple_of(r * width0, width0), width0)]
        xp[r + 1, unit0:unit0 + width0] = block.T
        return carry

    lax.fori_loop(0, th, load_body, 0)
    xp[0, unit0:unit0 + width0] = move(xp[th, unit0:unit0 + width0], above)
    for r in range(th + 1):
        xp[r, 0:unit0] = move(xp[r, width0:width0 + unit0], left)

    bufs = (xp, y1, z1, y2, z2, y3, None)
    h, w, ci = th, tw, c0
    for layer in range(6):
        stride, bh, bw = BLOCKS[layer]
        co = widths[layer // 2]
        h, w = h // stride, w // stride
        conv(bufs[layer], w_refs[layer], stride, bh, bw, ci, co, h, w, layer == 0)
        scale, offset = stats(v_refs[layer], co, float(h * w * tiles))
        ci = co
        if layer < 5:
            normalise(scale, offset, co, h, w, bufs[layer + 1])
            halos(bufs[layer + 1], h, w, co, layer % 2 == 0)
        else:
            for i in range(h):
                for j in range(w):
                    val = jnp.maximum(acc_a[i, j * co:(j + 1) * co] * scale + offset, 0.0)
                    out_ref[:, i * w + j] = val.T.reshape(tiles, imgs, co).astype(jnp.bfloat16)


def pack_kernel(x_ref, out_ref):
    rows, tw, c0, count = x_ref.shape
    for r in range(rows):
        out_ref[:, r * tw * c0:(r + 1) * tw * c0] = x_ref[r].reshape(tw * c0, count).T


def pack(tile):
    count, th, tw, c0 = tile.shape
    return pl.pallas_call(
        pack_kernel,
        grid=(th // 2,),
        out_shape=jax.ShapeDtypeStruct((count, th * tw * c0), tile.dtype),
        in_specs=[pl.BlockSpec((2, tw, c0, count), lambda r: (r, 0, 0, 0))],
        out_specs=pl.BlockSpec((count, 2 * tw * c0), lambda r: (0, r)),
    )(tile.transpose(1, 2, 3, 0))


def encode(cfg, x, weights, affines):
    th, tw, c0, widths, grid_h, grid_w, imgs = cfg
    tiles = grid_h * grid_w
    lanes = tiles * imgs
    c1, c2, c3 = widths
    bf16, f32 = jnp.bfloat16, jnp.float32
    vmem = pl.BlockSpec(memory_space=pltpu.VMEM)
    h1, w1, h2, w2, h3, w3 = th // 2, tw // 2, th // 4, tw // 4, th // 8, tw // 8
    flops = 2 * 9 * lanes * (h1 * w1 * (c0 * c1 + c1 * c1) + h2 * w2 * (c1 * c2 + c2 * c2) + h3 * w3 * (c2 * c3 + c3 * c3)) * 4
    return pl.pallas_call(
        functools.partial(encoder_kernel, cfg),
        out_shape=jax.ShapeDtypeStruct((tiles, h3 * w3, imgs, c3), bf16),
        in_specs=[vmem] * 13,
        out_specs=vmem,
        scratch_shapes=[
            pltpu.VMEM((th + 1, (tw + 4) * c0, lanes), bf16),
            pltpu.VMEM((h1, w1 * c1, lanes), f32),
            pltpu.VMEM((h1 + 2, (w1 + 2) * c1, lanes), bf16),
            pltpu.VMEM((h1 + 1, (w1 + 1) * c1, lanes), bf16),
            pltpu.VMEM((h2 + 2, (w2 + 2) * c2, lanes), bf16),
            pltpu.VMEM((h2 + 1, (w2 + 1) * c2, lanes), bf16),
            pltpu.VMEM((h3 + 2, (w3 + 2) * c3, lanes), bf16),
            pltpu.VMEM((2, c3, lanes), f32),
        ],
        compiler_params=pltpu.CompilerParams(vmem_limit_bytes=60 * 1024 * 1024),
        cost_estimate=pl.CostEstimate(flops=flops, bytes_accessed=4 * 1024 * 1024, transcendentals=0),
    )(x, *weights, *affines)


def solution(mesh):
    grid_h = mesh.shape["h"]
    grid_w = mesh.shape["w"]
    tiles = grid_h * grid_w
    act_spec = P("batch", "h", "w")

    def local_forward(tile, *params):
        count, th, tw, c0 = tile.shape
        kernels, affines = params[0::2], params[1::2]
        widths = tuple(kernels[2 * s].shape[3] for s in range(3))
        weights = [block_weights(k, *BLOCKS[i], i == 0) for i, k in enumerate(kernels)]
        columns = [v.T for v in affines]
        imgs = count // tiles // CHUNKS
        cfg = (th, tw, c0, widths, grid_h, grid_w, imgs)
        rows = pack(tile).reshape(CHUNKS, tiles, imgs, th * tw * c0)
        outs = []
        for k in range(CHUNKS):
            got = lax.all_to_all(rows[k], ("w", "h"), 0, 0)
            res = encode(cfg, got.reshape(tiles * imgs, th * tw * c0), weights, columns)
            outs.append(lax.all_to_all(res, ("w", "h"), 0, 0))
        full = jnp.stack(outs)
        return full.transpose(0, 1, 3, 2, 4).reshape(count, th // 8, tw // 8, widths[2])

    return jax.shard_map(local_forward, mesh=mesh, in_specs=(act_spec,) + (P(),) * 12, out_specs=act_spec, check_vma=False)
```

```python
import functools

import jax
import jax.numpy as jnp
from jax import lax
from jax.experimental import pallas as pl
from jax.experimental.pallas import tpu as pltpu
from jax.sharding import PartitionSpec as P

NORM_GROUPS = 8
NORM_EPS = 1e-5
CHUNKS = 4
BLOCKS = ((2, 1, 8), (1, 2, 4), (2, 1, 2), (1, 2, 2), (2, 1, 2), (1, 1, 2))
MESH = pl.DeviceIdType.MESH
BF16, F32 = jnp.bfloat16, jnp.float32


def peer_step(count):
    step = max(count // 3, 1)
    while any(count % d == 0 and step % d == 0 for d in range(2, count + 1)):
        step += 1
    return step


def patch_shape(stride, bh, bw, first):
    rows = (bh - 1) * stride + 3
    cols = (bw - 1) * stride + 3
    if first:
        cols = bw * stride + 4
    return rows, cols


def encoder_kernel(cfg, x_ref, *refs):
    th, tw, c0, widths, grid_h, grid_w, imgs = cfg
    tiles = grid_h * grid_w
    lanes = tiles * imgs
    w_refs, v_refs = refs[0:6], refs[6:12]
    out_ref = refs[12]
    (xs, send_in, recv_in, send_out, t0, t1, t2, t3, t4, t5, affine, xp, acc_a, y1, z1, y2, z2, y3, s_ref,
     load_sem, in_send, in_recv, in_own, out_send, out_recv, out_own) = refs[13:]
    t_refs = (t0, t1, t2, t3, t4, t5)
    half = th // 2
    width0 = tw * c0
    unit0 = 4 * c0

    my_w, my_h = lax.axis_index("w"), lax.axis_index("h")
    me = my_w * grid_h + my_h
    others = tiles - 1
    step = peer_step(others)

    def peer(n):
        offset = lax.rem(n * step, others) + 1
        pw = lax.rem(my_w + offset // grid_h, grid_w)
        ph = lax.rem(my_h + lax.rem(offset, grid_h), grid_h)
        return pw, ph, pw * grid_h + ph

    def loop(lower, upper, body):
        def step_body(n, carry):
            body(n)
            return carry
        lax.fori_loop(lower, upper, step_body, 0)

    def load(k):
        return pltpu.make_async_copy(x_ref.at[:, :, :, pl.ds(pl.multiple_of(k * lanes, lanes), lanes)], xs.at[k], load_sem.at[k])

    loop(0, CHUNKS, lambda k: load(k).start())
    barrier = pltpu.get_barrier_semaphore()

    def greet(n):
        pw, ph, _ = peer(n)
        pl.semaphore_signal(barrier, inc=1, device_id={"w": pw, "h": ph}, device_id_type=MESH)

    loop(0, others, greet)

    def iota(shape, dim):
        return lax.broadcasted_iota(jnp.int32, shape, dim)

    both = 2 * lanes
    o, i = iota((both, both), 0), iota((both, both), 1)
    o_tile, o_half, o_img = o // (2 * imgs), (o // imgs) % 2, o % imgs
    pair = jnp.where(i == o_half * lanes + o_tile * imgs + o_img, 1.0, 0.0).astype(BF16)

    def pack(k):
        load(k).wait()
        for r in range(half):
            cat = jnp.concatenate([xs[k, r].reshape(width0, lanes), xs[k, r + half].reshape(width0, lanes)], axis=1)
            res = lax.dot_general(pair, cat, (((1,), (1,)), ((), ())), preferred_element_type=F32)
            send_in[k, :, :, r * width0:(r + 1) * width0] = res.reshape(tiles, 2 * imgs, width0).astype(BF16)

    def copy_in(k, n):
        pw, ph, p = peer(n)
        return pltpu.make_async_remote_copy(
            src_ref=send_in.at[k, p], dst_ref=recv_in.at[k, me], send_sem=in_send.at[k, n], recv_sem=in_recv.at[k, n],
            device_id={"w": pw, "h": ph}, device_id_type=MESH)

    def own_in(k):
        return pltpu.make_async_copy(send_in.at[k, me], recv_in.at[k, me], in_own.at[k])

    def copy_out(k, n):
        pw, ph, p = peer(n)
        return pltpu.make_async_remote_copy(
            src_ref=send_out.at[k, p], dst_ref=out_ref.at[k, me], send_sem=out_send.at[k, n], recv_sem=out_recv.at[k, n],
            device_id={"w": pw, "h": ph}, device_id_type=MESH)

    def own_out(k):
        return pltpu.make_async_copy(send_out.at[k, me], out_ref.at[k, me], out_own.at[k])

    def start(k, copy, own):
        loop(0, others, lambda n: copy(k, n).start())
        own(k).start()

    def wait(k, copy, own):
        loop(0, others, lambda n: copy(k, n).wait())
        own(k).wait()

    pack(0)
    pl.semaphore_wait(barrier, others)
    start(0, copy_in, own_in)

    def pack_body(k):
        pack(k)
        start(k, copy_in, own_in)

    loop(1, CHUNKS, pack_body)

    for layer, (stride, bh, bw) in enumerate(BLOCKS):
        w_ref = w_refs[layer]
        ci, co = w_ref.shape[2], w_ref.shape[3]
        rows, cols = patch_shape(stride, bh, bw, layer == 0)
        off = 3 if layer == 0 else 0
        bands = [jnp.concatenate([w_ref[dy, dx].astype(F32) for dx in range(3)], axis=0).T for dy in range(3)]
        for bi in range(bh):
            for bj in range(bw):
                parts, at = [], 0
                for dy in range(3):
                    begin = ((stride * bi + dy) * cols + off + stride * bj) * ci
                    if begin > at:
                        parts.append(jnp.zeros((co, begin - at), F32))
                    parts.append(bands[dy])
                    at = begin + 3 * ci
                if rows * cols * ci > at:
                    parts.append(jnp.zeros((co, rows * cols * ci - at), F32))
                t_refs[layer][(bi * bw + bj) * co:(bi * bw + bj + 1) * co] = jnp.concatenate(parts, axis=1).astype(BF16)
        for q in range(3):
            affine[layer, q, 0:co] = jnp.broadcast_to(v_refs[layer][q:q + 1], (lanes, co)).T

    src_l, dst_l = iota((lanes, lanes), 0), iota((lanes, lanes), 1)

    def perm(dh, dw):
        t = dst_l // imgs
        h, w = t % grid_h + dh, t // grid_h + dw
        inside = (h >= 0) & (h < grid_h) & (w >= 0) & (w < grid_w)
        want = (w * grid_h + h) * imgs + dst_l % imgs
        return jnp.where(inside & (src_l == want), 1.0, 0.0).astype(BF16)

    above, below, left, right = perm(-1, 0), perm(1, 0), perm(0, -1), perm(0, 1)
    same_image = jnp.where(src_l % imgs == dst_l % imgs, 1.0, 0.0)

    def move(value, matrix):
        return jnp.dot(value, matrix, preferred_element_type=F32).astype(BF16)

    def halos(buf, rows, cols, unit, both_sides):
        buf[0] = move(buf[rows], above)
        if both_sides:
            buf[rows + 1] = move(buf[1], below)
        for r in range(rows + (2 if both_sides else 1)):
            buf[r, 0:unit] = move(buf[r, cols * unit:(cols + 1) * unit], left)
            if both_sides:
                buf[r, (cols + 1) * unit:(cols + 2) * unit] = move(buf[r, unit:2 * unit], right)

    def conv(buf, w_ref, stride, bh, bw, ci, co, out_h, out_w, first):
        rows, cols = patch_shape(stride, bh, bw, first)
        s_ref[:, 0:co] = jnp.zeros((2, co, lanes), F32)
        far = out_h // 2

        def row_body(n, carry):
            for j in range(out_w // bw):
                start = j * bw * stride * ci
                patches = []
                for base in (n * bh, n * bh + far):
                    patches.append(jnp.concatenate([buf[base * stride + r, start:start + cols * ci] for r in range(rows)], axis=0))
                res = jnp.dot(w_ref[...], jnp.concatenate(patches, axis=1), preferred_element_type=F32)
                parts = [res[p * co:(p + 1) * co, q * lanes:(q + 1) * lanes] for p in range(bh * bw) for q in range(2)]
                s_ref[0, 0:co] += functools.reduce(jnp.add, parts)
                s_ref[1, 0:co] += functools.reduce(jnp.add, [p * p for p in parts])
                for b in range(bh):
                    for q in range(2):
                        acc_a[n * bh + b + q * far, j * bw * co:(j + 1) * bw * co] = res[b * bw * co:(b + 1) * bw * co, q * lanes:(q + 1) * lanes]
            return carry

        lax.fori_loop(0, far // bh, row_body, 0)

    def stats(layer, co, pixels):
        per = co // NORM_GROUPS
        group = jnp.where(iota((co, co), 0) // per == iota((co, co), 1) // per, 1.0, 0.0)
        hi = lax.Precision.HIGHEST
        tot = jnp.dot(s_ref[:, 0:co].reshape(2 * co, lanes), same_image, precision=hi, preferred_element_type=F32) / pixels
        mean_c, sq_c = tot[0:co], tot[co:2 * co]
        var_c = jnp.maximum(sq_c - mean_c * mean_c, 0.0)
        bias, gain, shift = affine[layer, 0, 0:co], affine[layer, 1, 0:co], affine[layer, 2, 0:co]
        mean_a = mean_c + bias
        m = jnp.dot(group, mean_a, precision=hi, preferred_element_type=F32) / per
        dev = mean_a - m
        q = jnp.dot(group, var_c + dev * dev, precision=hi, preferred_element_type=F32) / per
        scale = lax.rsqrt(q + NORM_EPS) * gain
        return scale, shift + (bias - m) * scale

    def normalise(scale, offset, co, out_h, out_w, dst_buf):
        def row_body(r, carry):
            for j in range(out_w):
                val = acc_a[r, j * co:(j + 1) * co]
                dst_buf[r + 1, (j + 1) * co:(j + 2) * co] = jnp.maximum(val * scale + offset, 0.0).astype(BF16)
            return carry

        lax.fori_loop(0, out_h, row_body, 0)

    bufs = (xp, y1, z1, y2, z2, y3)

    def chunk(k):
        wait(k, copy_in, own_in)
        for r in range(half):
            block = recv_in[k, :, :, r * width0:(r + 1) * width0].astype(F32).reshape(both, width0)
            res = jnp.dot(block.T.astype(BF16), pair, preferred_element_type=F32).astype(BF16)
            xp[r + 1, unit0:unit0 + width0] = res[:, 0:lanes]
            xp[r + 1 + half, unit0:unit0 + width0] = res[:, lanes:both]
        xp[0, unit0:unit0 + width0] = move(xp[th, unit0:unit0 + width0], above)
        for r in range(th + 1):
            xp[r, 0:unit0] = move(xp[r, width0:width0 + unit0], left)

        h, w, ci = th, tw, c0
        for layer in range(6):
            stride, bh, bw = BLOCKS[layer]
            co = widths[layer // 2]
            h, w = h // stride, w // stride
            conv(bufs[layer], t_refs[layer], stride, bh, bw, ci, co, h, w, layer == 0)
            scale, offset = stats(layer, co, float(h * w * tiles))
            ci = co
            if layer < 5:
                normalise(scale, offset, co, h, w, bufs[layer + 1])
                halos(bufs[layer + 1], h, w, co, layer % 2 == 0)

        def finish(p):
            r, j = p // w, p % w
            return jnp.maximum(acc_a[r, j * ci:(j + 1) * ci] * scale + offset, 0.0).astype(BF16)

        for p in range(h * w // 2):
            cat = jnp.concatenate([finish(p), finish(p + h * w // 2)], axis=1)
            res = lax.dot_general(pair, cat, (((1,), (1,)), ((), ())), preferred_element_type=F32)
            send_out[k, :, p] = res.reshape(tiles, 2 * imgs, ci).astype(BF16)
        start(k, copy_out, own_out)

    loop(0, CHUNKS, chunk)
    loop(0, CHUNKS, lambda k: wait(k, copy_out, own_out))


def encode(cfg, x, kernels, affines):
    th, tw, c0, widths, grid_h, grid_w, imgs = cfg
    tiles = grid_h * grid_w
    lanes = tiles * imgs
    c1, c2, c3 = widths
    vmem = pl.BlockSpec(memory_space=pltpu.VMEM)
    hbm = pl.BlockSpec(memory_space=pl.ANY)
    h1, w1, h2, w2, h3, w3 = th // 2, tw // 2, th // 4, tw // 4, th // 8, tw // 8
    tables = []
    for layer, (stride, bh, bw) in enumerate(BLOCKS):
        rows, cols = patch_shape(stride, bh, bw, layer == 0)
        tables.append(pltpu.VMEM((bh * bw * kernels[layer].shape[3], rows * cols * kernels[layer].shape[2]), BF16))
    dma = pltpu.SemaphoreType.DMA
    return pl.pallas_call(
        functools.partial(encoder_kernel, cfg),
        out_shape=jax.ShapeDtypeStruct((CHUNKS, tiles, h3 * w3 // 2, 2 * imgs, c3), BF16),
        in_specs=[hbm] + [vmem] * 12,
        out_specs=hbm,
        scratch_shapes=[
            pltpu.VMEM((CHUNKS, th, tw, c0, lanes), BF16),
            pltpu.VMEM((CHUNKS, tiles, 2 * imgs, th * tw * c0 // 2), BF16),
            pltpu.VMEM((CHUNKS, tiles, 2 * imgs, th * tw * c0 // 2), BF16),
            pltpu.VMEM((CHUNKS, tiles, h3 * w3 // 2, 2 * imgs, c3), BF16),
            *tables,
            pltpu.VMEM((6, 3, c3, lanes), F32),
            pltpu.VMEM((th + 1, (tw + 4) * c0, lanes), BF16),
            pltpu.VMEM((h1, w1 * c1, lanes), F32),
            pltpu.VMEM((h1 + 2, (w1 + 2) * c1, lanes), BF16),
            pltpu.VMEM((h1 + 1, (w1 + 1) * c1, lanes), BF16),
            pltpu.VMEM((h2 + 2, (w2 + 2) * c2, lanes), BF16),
            pltpu.VMEM((h2 + 1, (w2 + 1) * c2, lanes), BF16),
            pltpu.VMEM((h3 + 2, (w3 + 2) * c3, lanes), BF16),
            pltpu.VMEM((2, c3, lanes), F32),
            dma((CHUNKS,)),
            dma((CHUNKS, tiles - 1)), dma((CHUNKS, tiles - 1)), dma((CHUNKS,)),
            dma((CHUNKS, tiles - 1)), dma((CHUNKS, tiles - 1)), dma((CHUNKS,)),
        ],
        compiler_params=pltpu.CompilerParams(vmem_limit_bytes=63 * 1024 * 1024, collective_id=0, has_side_effects=True),
    )(x, *kernels, *affines)


def solution(mesh):
    grid_h = mesh.shape["h"]
    grid_w = mesh.shape["w"]
    tiles = grid_h * grid_w
    act_spec = P("batch", "h", "w")

    def local_forward(tile, *params):
        count, th, tw, c0 = tile.shape
        kernels, affines = params[0::2], params[1::2]
        widths = tuple(kernels[2 * s].shape[3] for s in range(3))
        cfg = (th, tw, c0, widths, grid_h, grid_w, count // tiles // CHUNKS)
        res = encode(cfg, tile.transpose(1, 2, 3, 0), kernels, affines)
        imgs = count // tiles // CHUNKS
        res = res.reshape(CHUNKS, tiles, -1, 2, imgs, widths[2])
        return res.transpose(0, 1, 4, 3, 2, 5).reshape(count, th // 8, tw // 8, widths[2])

    return jax.shard_map(local_forward, mesh=mesh, in_specs=(act_spec,) + (P(),) * 12, out_specs=act_spec, check_vma=False)
```

```python
import functools

import jax
import jax.numpy as jnp
from jax import lax
from jax.experimental import pallas as pl
from jax.experimental.pallas import tpu as pltpu
from jax.sharding import PartitionSpec as P

NORM_GROUPS = 8
NORM_EPS = 1e-5
CHUNKS = 4
BLOCKS = ((2, 1, 8), (1, 2, 4), (2, 1, 2), (1, 2, 2), (2, 1, 2), (1, 1, 2))
MESH = pl.DeviceIdType.MESH
BF16, F32 = jnp.bfloat16, jnp.float32


def peer_step(count):
    step = max(count // 3, 1)
    while any(count % d == 0 and step % d == 0 for d in range(2, count + 1)):
        step += 1
    return step


def patch_shape(stride, bh, bw, first):
    rows = (bh - 1) * stride + 3
    cols = (bw - 1) * stride + 3
    if first:
        cols = bw * stride + 4
    return rows, cols


def encoder_kernel(cfg, x_ref, *refs):
    th, tw, c0, widths, grid_h, grid_w, imgs = cfg
    tiles = grid_h * grid_w
    lanes = tiles * imgs
    w_refs, v_refs = refs[0:6], refs[6:12]
    out_ref = refs[12]
    (xs, send_in, recv_in, send_out, t0, t1, t2, t3, t4, t5, affine, xp, acc_a, y1, z1, y2, z2, y3, s_ref,
     load_sem, in_send, in_recv, in_own, out_send, out_recv, out_own) = refs[13:]
    t_refs = (t0, t1, t2, t3, t4, t5)
    half = th // 2
    width0 = tw * c0
    unit0 = 4 * c0

    my_w, my_h = lax.axis_index("w"), lax.axis_index("h")
    me = my_w * grid_h + my_h
    others = tiles - 1
    step = peer_step(others)

    def peer(n):
        offset = lax.rem(n * step, others) + 1
        pw = lax.rem(my_w + offset // grid_h, grid_w)
        ph = lax.rem(my_h + lax.rem(offset, grid_h), grid_h)
        return pw, ph, pw * grid_h + ph

    def loop(lower, upper, body):
        def step_body(n, carry):
            body(n)
            return carry
        lax.fori_loop(lower, upper, step_body, 0)

    def load(k):
        return pltpu.make_async_copy(x_ref.at[:, :, :, pl.ds(pl.multiple_of(k * lanes, lanes), lanes)], xs.at[k], load_sem.at[k])

    loop(0, CHUNKS, lambda k: load(k).start())
    barrier = pltpu.get_barrier_semaphore()

    def greet(n):
        pw, ph, _ = peer(n)
        pl.semaphore_signal(barrier, inc=1, device_id={"w": pw, "h": ph}, device_id_type=MESH)

    loop(0, others, greet)

    def iota(shape, dim):
        return lax.broadcasted_iota(jnp.int32, shape, dim)

    both = 2 * lanes
    o, i = iota((both, both), 0), iota((both, both), 1)
    o_tile, o_half, o_img = o // (2 * imgs), (o // imgs) % 2, o % imgs
    pair = jnp.where(i == o_half * lanes + o_tile * imgs + o_img, 1.0, 0.0).astype(BF16)

    def pack(k):
        load(k).wait()
        for r in range(half):
            cat = jnp.concatenate([xs[k, r].reshape(width0, lanes), xs[k, r + half].reshape(width0, lanes)], axis=1)
            res = lax.dot_general(pair, cat, (((1,), (1,)), ((), ())), preferred_element_type=F32)
            send_in[k, :, :, r * width0:(r + 1) * width0] = res.reshape(tiles, 2 * imgs, width0).astype(BF16)

    def copy_in(k, n):
        pw, ph, p = peer(n)
        return pltpu.make_async_remote_copy(
            src_ref=send_in.at[k, p], dst_ref=recv_in.at[k, me], send_sem=in_send.at[k, n], recv_sem=in_recv.at[k, n],
            device_id={"w": pw, "h": ph}, device_id_type=MESH)

    def own_in(k):
        return pltpu.make_async_copy(send_in.at[k, me], recv_in.at[k, me], in_own.at[k])

    def copy_out(k, n):
        pw, ph, p = peer(n)
        return pltpu.make_async_remote_copy(
            src_ref=send_out.at[k, p], dst_ref=out_ref.at[k, me], send_sem=out_send.at[k, n], recv_sem=out_recv.at[k, n],
            device_id={"w": pw, "h": ph}, device_id_type=MESH)

    def own_out(k):
        return pltpu.make_async_copy(send_out.at[k, me], out_ref.at[k, me], out_own.at[k])

    def start(k, copy, own):
        for n in range(others):
            copy(k, n).start()
        own(k).start()

    def wait(k, copy, own):
        loop(0, others, lambda n: copy(k, n).wait())
        own(k).wait()

    pack(0)
    pl.semaphore_wait(barrier, others)
    start(0, copy_in, own_in)

    def pack_body(k):
        pack(k)
        start(k, copy_in, own_in)

    loop(1, CHUNKS, pack_body)

    for layer, (stride, bh, bw) in enumerate(BLOCKS):
        w_ref = w_refs[layer]
        ci, co = w_ref.shape[2], w_ref.shape[3]
        rows, cols = patch_shape(stride, bh, bw, layer == 0)
        off = 3 if layer == 0 else 0
        bands = [jnp.concatenate([w_ref[dy, dx].astype(F32) for dx in range(3)], axis=0).T for dy in range(3)]
        for bi in range(bh):
            for bj in range(bw):
                parts, at = [], 0
                for dy in range(3):
                    begin = ((stride * bi + dy) * cols + off + stride * bj) * ci
                    if begin > at:
                        parts.append(jnp.zeros((co, begin - at), F32))
                    parts.append(bands[dy])
                    at = begin + 3 * ci
                if rows * cols * ci > at:
                    parts.append(jnp.zeros((co, rows * cols * ci - at), F32))
                t_refs[layer][(bi * bw + bj) * co:(bi * bw + bj + 1) * co] = jnp.concatenate(parts, axis=1).astype(BF16)
        for q in range(3):
            affine[layer, q, 0:co] = jnp.broadcast_to(v_refs[layer][q:q + 1], (lanes, co)).T

    src_l, dst_l = iota((lanes, lanes), 0), iota((lanes, lanes), 1)
    same_image = jnp.where(src_l % imgs == dst_l % imgs, 1.0, 0.0).astype(BF16)
    lane = iota((16, lanes), 1)
    lane_h, lane_w = (lane // imgs) % grid_h, lane // (imgs * grid_h)

    def mask(dh, dw):
        h, w = lane_h + dh, lane_w + dw
        inside = (h >= 0) & (h < grid_h) & (w >= 0) & (w < grid_w)
        return jnp.where(inside, 1.0, 0.0).astype(BF16)

    masks = {(dh, dw): mask(dh, dw) for dh in (-1, 0, 1) for dw in (-1, 0, 1) if (dh, dw) != (0, 0)}

    def take(value, dh, dw):
        shift = (-(dh + dw * grid_h) * imgs) % lanes
        moved = pltpu.roll(value, shift, 1).reshape(-1, 16, lanes)
        return (moved * masks[(dh, dw)][None]).reshape(value.shape)

    def halos(buf, rows, cols, unit, both_sides):
        sides = (-1, 0, 1) if both_sides else (-1, 0)
        for dh in sides:
            for dw in sides:
                if (dh, dw) == (0, 0):
                    continue
                src_r = {-1: (rows, rows + 1), 0: (1, rows + 1), 1: (1, 2)}[dh]
                dst_r = {-1: 0, 0: 1, 1: rows + 1}[dh]
                src_c = {-1: (cols, cols + 1), 0: (1, cols + 1), 1: (1, 2)}[dw]
                dst_c = {-1: 0, 0: 1, 1: cols + 1}[dw]
                span = (src_c[1] - src_c[0]) * unit
                for n in range(src_r[1] - src_r[0]):
                    value = buf[src_r[0] + n, src_c[0] * unit:src_c[1] * unit]
                    buf[dst_r + n, dst_c * unit:dst_c * unit + span] = take(value, dh, dw)

    def conv(buf, w_ref, stride, bh, bw, ci, co, out_h, out_w, first):
        rows, cols = patch_shape(stride, bh, bw, first)
        s_ref[:, 0:co] = jnp.zeros((2, co, lanes), F32)
        far = out_h // 2

        def row_body(n, carry):
            for j in range(out_w // bw):
                start = j * bw * stride * ci
                patches = []
                for base in (n * bh, n * bh + far):
                    patches.append(jnp.concatenate([buf[base * stride + r, start:start + cols * ci] for r in range(rows)], axis=0))
                res = jnp.dot(w_ref[...], jnp.concatenate(patches, axis=1), preferred_element_type=F32)
                parts = [res[p * co:(p + 1) * co, q * lanes:(q + 1) * lanes] for p in range(bh * bw) for q in range(2)]
                s_ref[0, 0:co] += functools.reduce(jnp.add, parts)
                s_ref[1, 0:co] += functools.reduce(jnp.add, [p * p for p in parts])
                for b in range(bh):
                    for q in range(2):
                        acc_a[n * bh + b + q * far, j * bw * co:(j + 1) * bw * co] = res[b * bw * co:(b + 1) * bw * co, q * lanes:(q + 1) * lanes]
            return carry

        lax.fori_loop(0, far // bh, row_body, 0)

    def group_sum(x, co):
        per = co // NORM_GROUPS
        span = max(per, 8)
        y = x.reshape(co // span, span, lanes)
        if per >= 8:
            return jnp.broadcast_to(jnp.sum(y, axis=1, keepdims=True), y.shape).reshape(co, lanes)
        row = iota((1, span, lanes), 1) // per
        res = jnp.zeros_like(y)
        for g in range(span // per):
            part = jnp.sum(jnp.where(row == g, y, 0.0), axis=1, keepdims=True)
            res = jnp.where(row == g, part, res)
        return res.reshape(co, lanes)

    def stats(layer, co, pixels):
        bias, gain, shift = affine[layer, 0, 0:co], affine[layer, 1, 0:co], affine[layer, 2, 0:co]
        s1, s2 = s_ref[0, 0:co], s_ref[1, 0:co]
        with_bias = pixels * bias
        part = jnp.concatenate([group_sum(s1 + with_bias, co), group_sum(s2 + bias * (2.0 * s1 + with_bias), co)], axis=0)
        p0 = part.astype(BF16)
        rest = part - p0.astype(F32)
        p1 = rest.astype(BF16)
        p2 = (rest - p1.astype(F32)).astype(BF16)
        tot = jnp.dot(jnp.concatenate([p0, p1, p2], axis=0), same_image, preferred_element_type=F32)
        tot = (tot[0:2 * co] + tot[2 * co:4 * co] + tot[4 * co:6 * co]) * (1.0 / (pixels * tiles * (co // NORM_GROUPS)))
        m = tot[0:co]
        q = jnp.maximum(tot[co:2 * co] - m * m, 0.0)
        scale = lax.rsqrt(q + NORM_EPS) * gain
        return scale, shift + (bias - m) * scale

    def normalise(scale, offset, co, out_h, out_w, dst_buf):
        def row_body(r, carry):
            for j in range(out_w):
                val = acc_a[r, j * co:(j + 1) * co]
                dst_buf[r + 1, (j + 1) * co:(j + 2) * co] = jnp.maximum(val * scale + offset, 0.0).astype(BF16)
            return carry

        lax.fori_loop(0, out_h, row_body, 0)

    bufs = (xp, y1, z1, y2, z2, y3)

    def chunk(k):
        wait(k, copy_in, own_in)
        for r in range(half):
            block = recv_in[k, :, :, r * width0:(r + 1) * width0].astype(F32).reshape(both, width0)
            res = jnp.dot(block.T.astype(BF16), pair, preferred_element_type=F32).astype(BF16)
            xp[r + 1, unit0:unit0 + width0] = res[:, 0:lanes]
            xp[r + 1 + half, unit0:unit0 + width0] = res[:, lanes:both]
        xp[0, unit0:unit0 + width0] = take(xp[th, unit0:unit0 + width0], -1, 0)
        xp[0, 0:unit0] = take(xp[th, width0:width0 + unit0], -1, -1)
        for r in range(1, th + 1):
            xp[r, 0:unit0] = take(xp[r, width0:width0 + unit0], 0, -1)

        h, w, ci = th, tw, c0
        for layer in range(6):
            stride, bh, bw = BLOCKS[layer]
            co = widths[layer // 2]
            h, w = h // stride, w // stride
            conv(bufs[layer], t_refs[layer], stride, bh, bw, ci, co, h, w, layer == 0)
            scale, offset = stats(layer, co, float(h * w))
            ci = co
            if layer < 5:
                normalise(scale, offset, co, h, w, bufs[layer + 1])
                halos(bufs[layer + 1], h, w, co, layer % 2 == 0)

        def finish(p):
            r, j = p // w, p % w
            return jnp.maximum(acc_a[r, j * ci:(j + 1) * ci] * scale + offset, 0.0).astype(BF16)

        for p in range(h * w // 2):
            cat = jnp.concatenate([finish(p), finish(p + h * w // 2)], axis=1)
            res = lax.dot_general(pair, cat, (((1,), (1,)), ((), ())), preferred_element_type=F32)
            send_out[k, :, p] = res.reshape(tiles, 2 * imgs, ci).astype(BF16)
        start(k, copy_out, own_out)

    loop(0, CHUNKS, chunk)
    loop(0, CHUNKS, lambda k: wait(k, copy_out, own_out))


def encode(cfg, x, kernels, affines):
    th, tw, c0, widths, grid_h, grid_w, imgs = cfg
    tiles = grid_h * grid_w
    lanes = tiles * imgs
    c1, c2, c3 = widths
    vmem = pl.BlockSpec(memory_space=pltpu.VMEM)
    hbm = pl.BlockSpec(memory_space=pl.ANY)
    h1, w1, h2, w2, h3, w3 = th // 2, tw // 2, th // 4, tw // 4, th // 8, tw // 8
    tables = []
    for layer, (stride, bh, bw) in enumerate(BLOCKS):
        rows, cols = patch_shape(stride, bh, bw, layer == 0)
        tables.append(pltpu.VMEM((bh * bw * kernels[layer].shape[3], rows * cols * kernels[layer].shape[2]), BF16))
    dma = pltpu.SemaphoreType.DMA
    return pl.pallas_call(
        functools.partial(encoder_kernel, cfg),
        out_shape=jax.ShapeDtypeStruct((CHUNKS, tiles, h3 * w3 // 2, 2 * imgs, c3), BF16),
        in_specs=[hbm] + [vmem] * 12,
        out_specs=hbm,
        scratch_shapes=[
            pltpu.VMEM((CHUNKS, th, tw, c0, lanes), BF16),
            pltpu.VMEM((CHUNKS, tiles, 2 * imgs, th * tw * c0 // 2), BF16),
            pltpu.VMEM((CHUNKS, tiles, 2 * imgs, th * tw * c0 // 2), BF16),
            pltpu.VMEM((CHUNKS, tiles, h3 * w3 // 2, 2 * imgs, c3), BF16),
            *tables,
            pltpu.VMEM((6, 3, c3, lanes), F32),
            pltpu.VMEM((th + 1, (tw + 4) * c0, lanes), BF16),
            pltpu.VMEM((h1, w1 * c1, lanes), F32),
            pltpu.VMEM((h1 + 2, (w1 + 2) * c1, lanes), BF16),
            pltpu.VMEM((h1 + 1, (w1 + 1) * c1, lanes), BF16),
            pltpu.VMEM((h2 + 2, (w2 + 2) * c2, lanes), BF16),
            pltpu.VMEM((h2 + 1, (w2 + 1) * c2, lanes), BF16),
            pltpu.VMEM((h3 + 2, (w3 + 2) * c3, lanes), BF16),
            pltpu.VMEM((2, c3, lanes), F32),
            dma((CHUNKS,)),
            dma((CHUNKS, tiles - 1)), dma((CHUNKS, tiles - 1)), dma((CHUNKS,)),
            dma((CHUNKS, tiles - 1)), dma((CHUNKS, tiles - 1)), dma((CHUNKS,)),
        ],
        compiler_params=pltpu.CompilerParams(vmem_limit_bytes=63 * 1024 * 1024, collective_id=0, has_side_effects=True),
    )(x, *kernels, *affines)


def solution(mesh):
    grid_h = mesh.shape["h"]
    grid_w = mesh.shape["w"]
    tiles = grid_h * grid_w
    act_spec = P("batch", "h", "w")

    def local_forward(tile, *params):
        count, th, tw, c0 = tile.shape
        kernels, affines = params[0::2], params[1::2]
        widths = tuple(kernels[2 * s].shape[3] for s in range(3))
        cfg = (th, tw, c0, widths, grid_h, grid_w, count // tiles // CHUNKS)
        res = encode(cfg, tile.transpose(1, 2, 3, 0), kernels, affines)
        imgs = count // tiles // CHUNKS
        res = res.reshape(CHUNKS, tiles, -1, 2, imgs, widths[2])
        return res.transpose(0, 1, 4, 3, 2, 5).reshape(count, th // 8, tw // 8, widths[2])

    return jax.shard_map(local_forward, mesh=mesh, in_specs=(act_spec,) + (P(),) * 12, out_specs=act_spec, check_vma=False)
```

```python
import functools

import jax
import jax.numpy as jnp
from jax import lax
from jax.experimental import pallas as pl
from jax.experimental.pallas import tpu as pltpu
from jax.sharding import PartitionSpec as P

NORM_GROUPS = 8
NORM_EPS = 1e-5
CHUNKS = 4
BLOCKS = ((2, 1, 8), (1, 2, 4), (2, 1, 2), (1, 2, 2), (2, 1, 2), (1, 1, 2))
MESH = pl.DeviceIdType.MESH
BF16, F32 = jnp.bfloat16, jnp.float32


def send_order(grid_w, grid_h):
    def ring(d, size):
        return min(d, size - d)

    def hops(n):
        dw, dh = n // grid_h, n % grid_h
        return ring(dw, grid_w) + ring(dh // 2, grid_h // 2)

    return sorted(range(1, grid_w * grid_h), key=lambda n: -hops(n))


def patch_shape(stride, bh, bw, first):
    rows = (bh - 1) * stride + 3
    cols = (bw - 1) * stride + 3
    if first:
        cols = bw * stride + 4
    return rows, cols


def encoder_kernel(cfg, x_ref, *refs):
    th, tw, c0, widths, grid_h, grid_w, imgs = cfg
    tiles = grid_h * grid_w
    lanes = tiles * imgs
    param_refs = refs[0:12]
    out_ref = refs[12]
    (xs, send_in, recv_in, send_out, t0, t1, t2, t3, t4, t5, *rest) = refs[13:]
    param_bufs = rest[0:12]
    (affine, xp, acc_a, y1, z1, y2, z2, y3, s_ref,
     load_sem, param_sem, in_send, in_recv, in_own, out_send, out_recv, out_own) = rest[12:]
    w_refs, v_refs = param_bufs[0:6], param_bufs[6:12]
    t_refs = (t0, t1, t2, t3, t4, t5)
    half = th // 2
    width0 = tw * c0
    unit0 = 4 * c0

    my_w, my_h = lax.axis_index("w"), lax.axis_index("h")
    me = my_w * grid_h + my_h
    others = tiles - 1

    def peer(n):
        offset = n + 1
        pw = lax.rem(my_w + offset // grid_h, grid_w)
        ph = lax.rem(my_h + lax.rem(offset, grid_h), grid_h)
        return pw, ph, pw * grid_h + ph

    def loop(lower, upper, body):
        def step_body(n, carry):
            body(n)
            return carry
        lax.fori_loop(lower, upper, step_body, 0)

    def load(k):
        return pltpu.make_async_copy(x_ref.at[:, :, :, pl.ds(pl.multiple_of(k * lanes, lanes), lanes)], xs.at[k], load_sem.at[k])

    loop(0, CHUNKS, lambda k: load(k).start())
    params = [pltpu.make_async_copy(param_refs[n], param_bufs[n], param_sem.at[n]) for n in range(12)]
    for param in params:
        param.start()
    barrier = pltpu.get_barrier_semaphore()

    def greet(n):
        pw, ph, _ = peer(n)
        pl.semaphore_signal(barrier, inc=1, device_id={"w": pw, "h": ph}, device_id_type=MESH)

    loop(0, others, greet)

    def iota(shape, dim):
        return lax.broadcasted_iota(jnp.int32, shape, dim)

    both = 2 * lanes
    o, i = iota((both, both), 0), iota((both, both), 1)
    o_tile, o_half, o_img = o // (2 * imgs), (o // imgs) % 2, o % imgs
    pair = jnp.where(i == o_half * lanes + o_tile * imgs + o_img, 1.0, 0.0).astype(BF16)

    def pack(k):
        load(k).wait()
        for r in range(half):
            cat = jnp.concatenate([xs[k, r].reshape(width0, lanes), xs[k, r + half].reshape(width0, lanes)], axis=1)
            res = lax.dot_general(pair, cat, (((1,), (1,)), ((), ())), preferred_element_type=F32)
            send_in[k, :, :, r * width0:(r + 1) * width0] = res.reshape(tiles, 2 * imgs, width0).astype(BF16)

    def copy_in(k, n):
        pw, ph, p = peer(n)
        return pltpu.make_async_remote_copy(
            src_ref=send_in.at[k, p], dst_ref=recv_in.at[k, me], send_sem=in_send.at[k, n], recv_sem=in_recv.at[k, n],
            device_id={"w": pw, "h": ph}, device_id_type=MESH)

    def own_in(k):
        return pltpu.make_async_copy(send_in.at[k, me], recv_in.at[k, me], in_own.at[k])

    def copy_out(k, n):
        pw, ph, p = peer(n)
        return pltpu.make_async_remote_copy(
            src_ref=send_out.at[k, p], dst_ref=out_ref.at[k, me], send_sem=out_send.at[k, n], recv_sem=out_recv.at[k, n],
            device_id={"w": pw, "h": ph}, device_id_type=MESH)

    def own_out(k):
        return pltpu.make_async_copy(send_out.at[k, me], out_ref.at[k, me], out_own.at[k])

    def start(k, copy, own):
        for offset in send_order(grid_w, grid_h):
            copy(k, offset - 1).start()
        own(k).start()

    def wait(k, copy, own):
        loop(0, others, lambda n: copy(k, n).wait())
        own(k).wait()

    pack(0)
    pl.semaphore_wait(barrier, others)
    start(0, copy_in, own_in)

    def pack_body(k):
        pack(k)
        start(k, copy_in, own_in)

    loop(1, CHUNKS, pack_body)

    for param in params:
        param.wait()
    for layer, (stride, bh, bw) in enumerate(BLOCKS):
        w_ref = w_refs[layer]
        ci, co = w_ref.shape[2], w_ref.shape[3]
        rows, cols = patch_shape(stride, bh, bw, layer == 0)
        off = 3 if layer == 0 else 0
        bands = [jnp.concatenate([w_ref[dy, dx].astype(F32) for dx in range(3)], axis=0).T for dy in range(3)]
        for bi in range(bh):
            for bj in range(bw):
                parts, at = [], 0
                for dy in range(3):
                    begin = ((stride * bi + dy) * cols + off + stride * bj) * ci
                    if begin > at:
                        parts.append(jnp.zeros((co, begin - at), F32))
                    parts.append(bands[dy])
                    at = begin + 3 * ci
                if rows * cols * ci > at:
                    parts.append(jnp.zeros((co, rows * cols * ci - at), F32))
                t_refs[layer][(bi * bw + bj) * co:(bi * bw + bj + 1) * co] = jnp.concatenate(parts, axis=1).astype(BF16)
        for q in range(3):
            affine[layer, q, 0:co] = jnp.broadcast_to(v_refs[layer][q:q + 1], (lanes, co)).T

    src_l, dst_l = iota((lanes, lanes), 0), iota((lanes, lanes), 1)
    same_image = jnp.where(src_l % imgs == dst_l % imgs, 1.0, 0.0).astype(BF16)
    lane = iota((16, lanes), 1)
    lane_h, lane_w = (lane // imgs) % grid_h, lane // (imgs * grid_h)

    def mask(dh, dw):
        h, w = lane_h + dh, lane_w + dw
        inside = (h >= 0) & (h < grid_h) & (w >= 0) & (w < grid_w)
        return jnp.where(inside, 1.0, 0.0).astype(BF16)

    masks = {(dh, dw): mask(dh, dw) for dh in (-1, 0, 1) for dw in (-1, 0, 1) if (dh, dw) != (0, 0)}

    def take(value, dh, dw):
        shift = (-(dh + dw * grid_h) * imgs) % lanes
        moved = pltpu.roll(value, shift, 1).reshape(-1, 16, lanes)
        return (moved * masks[(dh, dw)][None]).reshape(value.shape)

    def halos(buf, rows, cols, unit, both_sides):
        sides = (-1, 0, 1) if both_sides else (-1, 0)
        for dh in sides:
            for dw in sides:
                if (dh, dw) == (0, 0):
                    continue
                src_r = {-1: (rows, rows + 1), 0: (1, rows + 1), 1: (1, 2)}[dh]
                dst_r = {-1: 0, 0: 1, 1: rows + 1}[dh]
                src_c = {-1: (cols, cols + 1), 0: (1, cols + 1), 1: (1, 2)}[dw]
                dst_c = {-1: 0, 0: 1, 1: cols + 1}[dw]
                span = (src_c[1] - src_c[0]) * unit
                for n in range(src_r[1] - src_r[0]):
                    value = buf[src_r[0] + n, src_c[0] * unit:src_c[1] * unit]
                    buf[dst_r + n, dst_c * unit:dst_c * unit + span] = take(value, dh, dw)

    def conv(buf, w_ref, stride, bh, bw, ci, co, out_h, out_w, first):
        rows, cols = patch_shape(stride, bh, bw, first)
        s_ref[:, 0:co] = jnp.zeros((2, co, lanes), F32)
        far = out_h // 2

        def row_body(n, carry):
            for j in range(out_w // bw):
                start = j * bw * stride * ci
                patches = []
                for base in (n * bh, n * bh + far):
                    patches.append(jnp.concatenate([buf[base * stride + r, start:start + cols * ci] for r in range(rows)], axis=0))
                res = jnp.dot(w_ref[...], jnp.concatenate(patches, axis=1), preferred_element_type=F32)
                parts = [res[p * co:(p + 1) * co, q * lanes:(q + 1) * lanes] for p in range(bh * bw) for q in range(2)]
                s_ref[0, 0:co] += functools.reduce(jnp.add, parts)
                s_ref[1, 0:co] += functools.reduce(jnp.add, [p * p for p in parts])
                for b in range(bh):
                    for q in range(2):
                        acc_a[n * bh + b + q * far, j * bw * co:(j + 1) * bw * co] = res[b * bw * co:(b + 1) * bw * co, q * lanes:(q + 1) * lanes]
            return carry

        lax.fori_loop(0, far // bh, row_body, 0)

    def group_sum(x, co):
        per = co // NORM_GROUPS
        span = max(per, 8)
        y = x.reshape(co // span, span, lanes)
        if per >= 8:
            return jnp.broadcast_to(jnp.sum(y, axis=1, keepdims=True), y.shape).reshape(co, lanes)
        row = iota((1, span, lanes), 1) // per
        res = jnp.zeros_like(y)
        for g in range(span // per):
            part = jnp.sum(jnp.where(row == g, y, 0.0), axis=1, keepdims=True)
            res = jnp.where(row == g, part, res)
        return res.reshape(co, lanes)

    def stats(layer, co, pixels):
        bias, gain, shift = affine[layer, 0, 0:co], affine[layer, 1, 0:co], affine[layer, 2, 0:co]
        s1, s2 = s_ref[0, 0:co], s_ref[1, 0:co]
        with_bias = pixels * bias
        part = jnp.concatenate([group_sum(s1 + with_bias, co), group_sum(s2 + bias * (2.0 * s1 + with_bias), co)], axis=0)
        p0 = part.astype(BF16)
        rest = part - p0.astype(F32)
        p1 = rest.astype(BF16)
        p2 = (rest - p1.astype(F32)).astype(BF16)
        tot = jnp.dot(jnp.concatenate([p0, p1, p2], axis=0), same_image, preferred_element_type=F32)
        tot = (tot[0:2 * co] + tot[2 * co:4 * co] + tot[4 * co:6 * co]) * (1.0 / (pixels * tiles * (co // NORM_GROUPS)))
        m = tot[0:co]
        q = jnp.maximum(tot[co:2 * co] - m * m, 0.0)
        scale = lax.rsqrt(q + NORM_EPS) * gain
        return scale, shift + (bias - m) * scale

    def normalise(scale, offset, co, out_h, out_w, dst_buf):
        def row_body(r, carry):
            for j in range(out_w):
                val = acc_a[r, j * co:(j + 1) * co]
                dst_buf[r + 1, (j + 1) * co:(j + 2) * co] = jnp.maximum(val * scale + offset, 0.0).astype(BF16)
            return carry

        lax.fori_loop(0, out_h, row_body, 0)

    bufs = (xp, y1, z1, y2, z2, y3)

    def chunk(k):
        wait(k, copy_in, own_in)
        for r in range(half):
            block = recv_in[k, :, :, r * width0:(r + 1) * width0].astype(F32).reshape(both, width0)
            res = jnp.dot(block.T.astype(BF16), pair, preferred_element_type=F32).astype(BF16)
            xp[r + 1, unit0:unit0 + width0] = res[:, 0:lanes]
            xp[r + 1 + half, unit0:unit0 + width0] = res[:, lanes:both]
        xp[0, unit0:unit0 + width0] = take(xp[th, unit0:unit0 + width0], -1, 0)
        xp[0, 0:unit0] = take(xp[th, width0:width0 + unit0], -1, -1)
        for r in range(1, th + 1):
            xp[r, 0:unit0] = take(xp[r, width0:width0 + unit0], 0, -1)

        h, w, ci = th, tw, c0
        for layer in range(6):
            stride, bh, bw = BLOCKS[layer]
            co = widths[layer // 2]
            h, w = h // stride, w // stride
            conv(bufs[layer], t_refs[layer], stride, bh, bw, ci, co, h, w, layer == 0)
            scale, offset = stats(layer, co, float(h * w))
            ci = co
            if layer < 5:
                normalise(scale, offset, co, h, w, bufs[layer + 1])
                halos(bufs[layer + 1], h, w, co, layer % 2 == 0)

        def finish(p):
            r, j = p // w, p % w
            return jnp.maximum(acc_a[r, j * ci:(j + 1) * ci] * scale + offset, 0.0).astype(BF16)

        for p in range(h * w // 2):
            cat = jnp.concatenate([finish(p), finish(p + h * w // 2)], axis=1)
            res = lax.dot_general(pair, cat, (((1,), (1,)), ((), ())), preferred_element_type=F32)
            send_out[k, :, p] = res.reshape(tiles, 2 * imgs, ci).astype(BF16)
        start(k, copy_out, own_out)

    loop(0, CHUNKS, chunk)
    loop(0, CHUNKS, lambda k: wait(k, copy_out, own_out))


def encode(cfg, x, kernels, affines):
    th, tw, c0, widths, grid_h, grid_w, imgs = cfg
    tiles = grid_h * grid_w
    lanes = tiles * imgs
    c1, c2, c3 = widths
    h1, w1, h2, w2, h3, w3 = th // 2, tw // 2, th // 4, tw // 4, th // 8, tw // 8
    tables = []
    for layer, (stride, bh, bw) in enumerate(BLOCKS):
        rows, cols = patch_shape(stride, bh, bw, layer == 0)
        tables.append(pltpu.VMEM((bh * bw * kernels[layer].shape[3], rows * cols * kernels[layer].shape[2]), BF16))
    dma = pltpu.SemaphoreType.DMA
    return pl.pallas_call(
        functools.partial(encoder_kernel, cfg),
        out_shape=jax.ShapeDtypeStruct((CHUNKS, tiles, h3 * w3 // 2, 2 * imgs, c3), BF16),
        in_specs=[pl.BlockSpec(memory_space=pltpu.HBM)] * 13,
        out_specs=pl.BlockSpec(memory_space=pl.ANY),
        scratch_shapes=[
            pltpu.VMEM((CHUNKS, th, tw, c0, lanes), BF16),
            pltpu.VMEM((CHUNKS, tiles, 2 * imgs, th * tw * c0 // 2), BF16),
            pltpu.VMEM((CHUNKS, tiles, 2 * imgs, th * tw * c0 // 2), BF16),
            pltpu.VMEM((CHUNKS, tiles, h3 * w3 // 2, 2 * imgs, c3), BF16),
            *tables,
            *[pltpu.VMEM(p.shape, p.dtype) for p in (*kernels, *affines)],
            pltpu.VMEM((6, 3, c3, lanes), F32),
            pltpu.VMEM((th + 1, (tw + 4) * c0, lanes), BF16),
            pltpu.VMEM((h1, w1 * c1, lanes), F32),
            pltpu.VMEM((h1 + 2, (w1 + 2) * c1, lanes), BF16),
            pltpu.VMEM((h1 + 1, (w1 + 1) * c1, lanes), BF16),
            pltpu.VMEM((h2 + 2, (w2 + 2) * c2, lanes), BF16),
            pltpu.VMEM((h2 + 1, (w2 + 1) * c2, lanes), BF16),
            pltpu.VMEM((h3 + 2, (w3 + 2) * c3, lanes), BF16),
            pltpu.VMEM((2, c3, lanes), F32),
            dma((CHUNKS,)), dma((12,)),
            dma((CHUNKS, tiles - 1)), dma((CHUNKS, tiles - 1)), dma((CHUNKS,)),
            dma((CHUNKS, tiles - 1)), dma((CHUNKS, tiles - 1)), dma((CHUNKS,)),
        ],
        compiler_params=pltpu.CompilerParams(vmem_limit_bytes=40 * 1024 * 1024, collective_id=0, has_side_effects=True),
    )(*[pltpu.with_memory_space_constraint(p, pltpu.HBM) for p in (x, *kernels, *affines)])


def solution(mesh):
    grid_h = mesh.shape["h"]
    grid_w = mesh.shape["w"]
    tiles = grid_h * grid_w
    act_spec = P("batch", "h", "w")

    def local_forward(tile, *params):
        count, th, tw, c0 = tile.shape
        kernels, affines = params[0::2], params[1::2]
        widths = tuple(kernels[2 * s].shape[3] for s in range(3))
        cfg = (th, tw, c0, widths, grid_h, grid_w, count // tiles // CHUNKS)
        res = encode(cfg, tile.transpose(1, 2, 3, 0), kernels, affines)
        imgs = count // tiles // CHUNKS
        res = res.reshape(CHUNKS, tiles, -1, 2, imgs, widths[2])
        return res.transpose(0, 1, 4, 3, 2, 5).reshape(count, th // 8, tw // 8, widths[2])

    return jax.shard_map(local_forward, mesh=mesh, in_specs=(act_spec,) + (P(),) * 12, out_specs=act_spec, check_vma=False)
```

```python
import functools
import random

import jax
import jax.numpy as jnp
from jax import lax
from jax.experimental import pallas as pl
from jax.experimental.pallas import tpu as pltpu
from jax.sharding import PartitionSpec as P

NORM_GROUPS = 8
NORM_EPS = 1e-5
CHUNKS = 4
SEED = 12
BLOCKS = ((2, 1, 8), (1, 2, 4), (2, 1, 2), (1, 2, 2), (2, 1, 2), (1, 1, 2))
MESH = pl.DeviceIdType.MESH
BF16, F32 = jnp.bfloat16, jnp.float32


def send_order(grid_w, grid_h):
    order = list(range(1, grid_w * grid_h))
    random.Random(SEED).shuffle(order)
    return order


def patch_shape(stride, bh, bw, first):
    rows = (bh - 1) * stride + 3
    cols = (bw - 1) * stride + 3
    if first:
        cols = bw * stride + 4
    return rows, cols


def encoder_kernel(cfg, x_ref, *refs):
    th, tw, c0, widths, grid_h, grid_w, imgs = cfg
    tiles = grid_h * grid_w
    lanes = tiles * imgs
    param_refs = refs[0:12]
    out_ref = refs[12]
    (xs, send_in, recv_in, send_out, t0, t1, t2, t3, t4, t5, *rest) = refs[13:]
    param_bufs = rest[0:12]
    (affine, xp, acc_a, y1, z1, y2, z2, y3, s_ref,
     row_sem, load_sem, param_sem, in_send, in_recv, in_own, out_send, out_recv, out_own) = rest[12:]
    w_refs, v_refs = param_bufs[0:6], param_bufs[6:12]
    t_refs = (t0, t1, t2, t3, t4, t5)
    half = th // 2
    width0 = tw * c0
    unit0 = 4 * c0

    my_w, my_h = lax.axis_index("w"), lax.axis_index("h")
    me = my_w * grid_h + my_h
    others = tiles - 1

    def peer(n):
        offset = n + 1
        pw = lax.rem(my_w + offset // grid_h, grid_w)
        ph = lax.rem(my_h + lax.rem(offset, grid_h), grid_h)
        return pw, ph, pw * grid_h + ph

    def loop(lower, upper, body):
        def step_body(n, carry):
            body(n)
            return carry
        lax.fori_loop(lower, upper, step_body, 0)

    def load(k):
        return pltpu.make_async_copy(x_ref.at[:, :, :, pl.ds(pl.multiple_of(k * lanes, lanes), lanes)], xs.at[k], load_sem.at[k])

    barrier = pltpu.get_barrier_semaphore()
    in_column = [dw * grid_h for dw in range(1, grid_w)]
    near = in_column + list(range(1, grid_h))

    def greet(semaphore, offset):
        pw, ph, _ = peer(offset - 1)
        pl.semaphore_signal(semaphore, inc=1, device_id={"w": pw, "h": ph}, device_id_type=MESH)

    for offset in near:
        greet(barrier, offset)
    loop(0, CHUNKS, lambda k: load(k).start())
    params = [pltpu.make_async_copy(param_refs[n], param_bufs[n], param_sem.at[n]) for n in range(12)]
    for param in params:
        param.start()
    pl.semaphore_wait(barrier, len(near))
    for offset in in_column:
        greet(row_sem, offset)

    def iota(shape, dim):
        return lax.broadcasted_iota(jnp.int32, shape, dim)

    both = 2 * lanes
    o, i = iota((both, both), 0), iota((both, both), 1)
    o_tile, o_half, o_img = o // (2 * imgs), (o // imgs) % 2, o % imgs
    pair = jnp.where(i == o_half * lanes + o_tile * imgs + o_img, 1.0, 0.0).astype(BF16)

    def pack(k):
        load(k).wait()
        for r in range(half):
            cat = jnp.concatenate([xs[k, r].reshape(width0, lanes), xs[k, r + half].reshape(width0, lanes)], axis=1)
            res = lax.dot_general(pair, cat, (((1,), (1,)), ((), ())), preferred_element_type=F32)
            send_in[k, :, :, r * width0:(r + 1) * width0] = res.reshape(tiles, 2 * imgs, width0).astype(BF16)

    def copy_in(k, n):
        pw, ph, p = peer(n)
        return pltpu.make_async_remote_copy(
            src_ref=send_in.at[k, p], dst_ref=recv_in.at[k, me], send_sem=in_send.at[k, n], recv_sem=in_recv.at[k, n],
            device_id={"w": pw, "h": ph}, device_id_type=MESH)

    def own_in(k):
        return pltpu.make_async_copy(send_in.at[k, me], recv_in.at[k, me], in_own.at[k])

    def copy_out(k, n):
        pw, ph, p = peer(n)
        return pltpu.make_async_remote_copy(
            src_ref=send_out.at[k, p], dst_ref=out_ref.at[k, me], send_sem=out_send.at[k, n], recv_sem=out_recv.at[k, n],
            device_id={"w": pw, "h": ph}, device_id_type=MESH)

    def own_out(k):
        return pltpu.make_async_copy(send_out.at[k, me], out_ref.at[k, me], out_own.at[k])

    def start(k, copy, own):
        for offset in send_order(grid_w, grid_h):
            copy(k, offset - 1).start()
        own(k).start()

    def wait(k, copy, own):
        loop(0, others, lambda n: copy(k, n).wait())
        own(k).wait()

    pack(0)
    pl.semaphore_wait(row_sem, len(in_column))
    start(0, copy_in, own_in)

    def pack_body(k):
        pack(k)
        pl.when(k < CHUNKS - 1)(lambda: start(k, copy_in, own_in))

    loop(1, CHUNKS, pack_body)

    for param in params:
        param.wait()
    for layer, (stride, bh, bw) in enumerate(BLOCKS):
        w_ref = w_refs[layer]
        ci, co = w_ref.shape[2], w_ref.shape[3]
        rows, cols = patch_shape(stride, bh, bw, layer == 0)
        off = 3 if layer == 0 else 0
        bands = [jnp.concatenate([w_ref[dy, dx].astype(F32) for dx in range(3)], axis=0).T for dy in range(3)]
        for bi in range(bh):
            for bj in range(bw):
                parts, at = [], 0
                for dy in range(3):
                    begin = ((stride * bi + dy) * cols + off + stride * bj) * ci
                    if begin > at:
                        parts.append(jnp.zeros((co, begin - at), F32))
                    parts.append(bands[dy])
                    at = begin + 3 * ci
                if rows * cols * ci > at:
                    parts.append(jnp.zeros((co, rows * cols * ci - at), F32))
                t_refs[layer][(bi * bw + bj) * co:(bi * bw + bj + 1) * co] = jnp.concatenate(parts, axis=1).astype(BF16)
        for q in range(3):
            affine[layer, q, 0:co] = jnp.broadcast_to(v_refs[layer][q:q + 1], (lanes, co)).T

    src_l, dst_l = iota((lanes, lanes), 0), iota((lanes, lanes), 1)
    same_image = jnp.where(src_l % imgs == dst_l % imgs, 1.0, 0.0).astype(BF16)
    lane = iota((16, lanes), 1)
    lane_h, lane_w = (lane // imgs) % grid_h, lane // (imgs * grid_h)

    def mask(dh, dw):
        h, w = lane_h + dh, lane_w + dw
        inside = (h >= 0) & (h < grid_h) & (w >= 0) & (w < grid_w)
        return jnp.where(inside, 1.0, 0.0).astype(BF16)

    masks = {(dh, dw): mask(dh, dw) for dh in (-1, 0, 1) for dw in (-1, 0, 1) if (dh, dw) != (0, 0)}

    def take(value, dh, dw):
        shift = (-(dh + dw * grid_h) * imgs) % lanes
        moved = pltpu.roll(value, shift, 1).reshape(-1, 16, lanes)
        return (moved * masks[(dh, dw)][None]).reshape(value.shape)

    def halos(buf, rows, cols, unit, both_sides):
        sides = (-1, 0, 1) if both_sides else (-1, 0)
        for dh in sides:
            for dw in sides:
                if (dh, dw) == (0, 0):
                    continue
                src_r = {-1: (rows, rows + 1), 0: (1, rows + 1), 1: (1, 2)}[dh]
                dst_r = {-1: 0, 0: 1, 1: rows + 1}[dh]
                src_c = {-1: (cols, cols + 1), 0: (1, cols + 1), 1: (1, 2)}[dw]
                dst_c = {-1: 0, 0: 1, 1: cols + 1}[dw]
                span = (src_c[1] - src_c[0]) * unit
                for n in range(src_r[1] - src_r[0]):
                    value = buf[src_r[0] + n, src_c[0] * unit:src_c[1] * unit]
                    buf[dst_r + n, dst_c * unit:dst_c * unit + span] = take(value, dh, dw)

    def conv(buf, w_ref, stride, bh, bw, ci, co, out_h, out_w, first):
        rows, cols = patch_shape(stride, bh, bw, first)
        s_ref[:, 0:co] = jnp.zeros((2, co, lanes), F32)
        far = out_h // 2

        def row_body(n, carry):
            for j in range(out_w // bw):
                start = j * bw * stride * ci
                patches = []
                for base in (n * bh, n * bh + far):
                    patches.append(jnp.concatenate([buf[base * stride + r, start:start + cols * ci] for r in range(rows)], axis=0))
                res = jnp.dot(w_ref[...], jnp.concatenate(patches, axis=1), preferred_element_type=F32)
                parts = [res[p * co:(p + 1) * co, q * lanes:(q + 1) * lanes] for p in range(bh * bw) for q in range(2)]
                s_ref[0, 0:co] += functools.reduce(jnp.add, parts)
                s_ref[1, 0:co] += functools.reduce(jnp.add, [p * p for p in parts])
                for b in range(bh):
                    for q in range(2):
                        acc_a[n * bh + b + q * far, j * bw * co:(j + 1) * bw * co] = res[b * bw * co:(b + 1) * bw * co, q * lanes:(q + 1) * lanes]
            return carry

        lax.fori_loop(0, far // bh, row_body, 0)

    def group_sum(x, co):
        per = co // NORM_GROUPS
        span = max(per, 8)
        y = x.reshape(co // span, span, lanes)
        if per >= 8:
            return jnp.broadcast_to(jnp.sum(y, axis=1, keepdims=True), y.shape).reshape(co, lanes)
        row = iota((1, span, lanes), 1) // per
        res = jnp.zeros_like(y)
        for g in range(span // per):
            part = jnp.sum(jnp.where(row == g, y, 0.0), axis=1, keepdims=True)
            res = jnp.where(row == g, part, res)
        return res.reshape(co, lanes)

    def stats(layer, co, pixels):
        bias, gain, shift = affine[layer, 0, 0:co], affine[layer, 1, 0:co], affine[layer, 2, 0:co]
        s1, s2 = s_ref[0, 0:co], s_ref[1, 0:co]
        with_bias = pixels * bias
        part = jnp.concatenate([group_sum(s1 + with_bias, co), group_sum(s2 + bias * (2.0 * s1 + with_bias), co)], axis=0)
        p0 = part.astype(BF16)
        rest = part - p0.astype(F32)
        p1 = rest.astype(BF16)
        p2 = (rest - p1.astype(F32)).astype(BF16)
        tot = jnp.dot(jnp.concatenate([p0, p1, p2], axis=0), same_image, preferred_element_type=F32)
        tot = (tot[0:2 * co] + tot[2 * co:4 * co] + tot[4 * co:6 * co]) * (1.0 / (pixels * tiles * (co // NORM_GROUPS)))
        m = tot[0:co]
        q = jnp.maximum(tot[co:2 * co] - m * m, 0.0)
        scale = lax.rsqrt(q + NORM_EPS) * gain
        return scale, shift + (bias - m) * scale

    def normalise(scale, offset, co, out_h, out_w, dst_buf):
        def row_body(r, carry):
            for j in range(out_w):
                val = acc_a[r, j * co:(j + 1) * co]
                dst_buf[r + 1, (j + 1) * co:(j + 2) * co] = jnp.maximum(val * scale + offset, 0.0).astype(BF16)
            return carry

        lax.fori_loop(0, out_h, row_body, 0)

    bufs = (xp, y1, z1, y2, z2, y3)

    def chunk(k):
        wait(k, copy_in, own_in)
        pl.when(k == 0)(lambda: start(CHUNKS - 1, copy_in, own_in))
        for r in range(half):
            block = recv_in[k, :, :, r * width0:(r + 1) * width0].astype(F32).reshape(both, width0)
            res = jnp.dot(block.T.astype(BF16), pair, preferred_element_type=F32).astype(BF16)
            xp[r + 1, unit0:unit0 + width0] = res[:, 0:lanes]
            xp[r + 1 + half, unit0:unit0 + width0] = res[:, lanes:both]
        xp[0, unit0:unit0 + width0] = take(xp[th, unit0:unit0 + width0], -1, 0)
        xp[0, 0:unit0] = take(xp[th, width0:width0 + unit0], -1, -1)
        for r in range(1, th + 1):
            xp[r, 0:unit0] = take(xp[r, width0:width0 + unit0], 0, -1)

        h, w, ci = th, tw, c0
        for layer in range(6):
            stride, bh, bw = BLOCKS[layer]
            co = widths[layer // 2]
            h, w = h // stride, w // stride
            conv(bufs[layer], t_refs[layer], stride, bh, bw, ci, co, h, w, layer == 0)
            scale, offset = stats(layer, co, float(h * w))
            ci = co
            if layer < 5:
                normalise(scale, offset, co, h, w, bufs[layer + 1])
                halos(bufs[layer + 1], h, w, co, layer % 2 == 0)

        def finish(p):
            r, j = p // w, p % w
            return jnp.maximum(acc_a[r, j * ci:(j + 1) * ci] * scale + offset, 0.0).astype(BF16)

        for p in range(h * w // 2):
            cat = jnp.concatenate([finish(p), finish(p + h * w // 2)], axis=1)
            res = lax.dot_general(pair, cat, (((1,), (1,)), ((), ())), preferred_element_type=F32)
            send_out[k, :, p] = res.reshape(tiles, 2 * imgs, ci).astype(BF16)
        start(k, copy_out, own_out)

    loop(0, CHUNKS, chunk)
    loop(0, CHUNKS, lambda k: wait(k, copy_out, own_out))


def encode(cfg, x, kernels, affines):
    th, tw, c0, widths, grid_h, grid_w, imgs = cfg
    tiles = grid_h * grid_w
    lanes = tiles * imgs
    c1, c2, c3 = widths
    h1, w1, h2, w2, h3, w3 = th // 2, tw // 2, th // 4, tw // 4, th // 8, tw // 8
    tables = []
    for layer, (stride, bh, bw) in enumerate(BLOCKS):
        rows, cols = patch_shape(stride, bh, bw, layer == 0)
        tables.append(pltpu.VMEM((bh * bw * kernels[layer].shape[3], rows * cols * kernels[layer].shape[2]), BF16))
    dma = pltpu.SemaphoreType.DMA
    return pl.pallas_call(
        functools.partial(encoder_kernel, cfg),
        out_shape=jax.ShapeDtypeStruct((CHUNKS, tiles, h3 * w3 // 2, 2 * imgs, c3), BF16),
        in_specs=[pl.BlockSpec(memory_space=pltpu.HBM)] * 13,
        out_specs=pl.BlockSpec(memory_space=pl.ANY),
        scratch_shapes=[
            pltpu.VMEM((CHUNKS, th, tw, c0, lanes), BF16),
            pltpu.VMEM((CHUNKS, tiles, 2 * imgs, th * tw * c0 // 2), BF16),
            pltpu.VMEM((CHUNKS, tiles, 2 * imgs, th * tw * c0 // 2), BF16),
            pltpu.VMEM((CHUNKS, tiles, h3 * w3 // 2, 2 * imgs, c3), BF16),
            *tables,
            *[pltpu.VMEM(p.shape, p.dtype) for p in (*kernels, *affines)],
            pltpu.VMEM((6, 3, c3, lanes), F32),
            pltpu.VMEM((th + 1, (tw + 4) * c0, lanes), BF16),
            pltpu.VMEM((h1, w1 * c1, lanes), F32),
            pltpu.VMEM((h1 + 2, (w1 + 2) * c1, lanes), BF16),
            pltpu.VMEM((h1 + 1, (w1 + 1) * c1, lanes), BF16),
            pltpu.VMEM((h2 + 2, (w2 + 2) * c2, lanes), BF16),
            pltpu.VMEM((h2 + 1, (w2 + 1) * c2, lanes), BF16),
            pltpu.VMEM((h3 + 2, (w3 + 2) * c3, lanes), BF16),
            pltpu.VMEM((2, c3, lanes), F32),
            pltpu.SemaphoreType.REGULAR, dma((CHUNKS,)), dma((12,)),
            dma((CHUNKS, tiles - 1)), dma((CHUNKS, tiles - 1)), dma((CHUNKS,)),
            dma((CHUNKS, tiles - 1)), dma((CHUNKS, tiles - 1)), dma((CHUNKS,)),
        ],
        compiler_params=pltpu.CompilerParams(vmem_limit_bytes=40 * 1024 * 1024, collective_id=0, has_side_effects=True),
    )(*[pltpu.with_memory_space_constraint(p, pltpu.HBM) for p in (x, *kernels, *affines)])


def solution(mesh):
    grid_h = mesh.shape["h"]
    grid_w = mesh.shape["w"]
    tiles = grid_h * grid_w
    act_spec = P("batch", "h", "w")

    def local_forward(tile, *params):
        count, th, tw, c0 = tile.shape
        kernels, affines = params[0::2], params[1::2]
        widths = tuple(kernels[2 * s].shape[3] for s in range(3))
        cfg = (th, tw, c0, widths, grid_h, grid_w, count // tiles // CHUNKS)
        res = encode(cfg, tile.transpose(1, 2, 3, 0), kernels, affines)
        imgs = count // tiles // CHUNKS
        res = res.reshape(CHUNKS, tiles, -1, 2, imgs, widths[2])
        return res.transpose(0, 1, 4, 3, 2, 5).reshape(count, th // 8, tw // 8, widths[2])

    return jax.shard_map(local_forward, mesh=mesh, in_specs=(act_spec,) + (P(),) * 12, out_specs=act_spec, check_vma=False)
```

```python
import functools
import random

import jax
import jax.numpy as jnp
from jax import lax
from jax.experimental import pallas as pl
from jax.experimental.pallas import tpu as pltpu
from jax.sharding import PartitionSpec as P

NORM_GROUPS = 8
NORM_EPS = 1e-5
CHUNKS = 4
SEED = 12
OUT_SEED = 3
BLOCKS = ((2, 1, 8), (1, 2, 4), (2, 1, 2), (1, 2, 2), (2, 1, 2), (1, 1, 2))
MESH = pl.DeviceIdType.MESH
BF16, F32 = jnp.bfloat16, jnp.float32


def send_order(grid_w, grid_h, seed=SEED):
    order = list(range(1, grid_w * grid_h))
    random.Random(seed).shuffle(order)
    return order


def patch_shape(stride, bh, bw, first):
    rows = (bh - 1) * stride + 3
    cols = (bw - 1) * stride + 3
    if first:
        cols = bw * stride + 4
    return rows, cols


def encoder_kernel(cfg, x_ref, *refs):
    th, tw, c0, widths, grid_h, grid_w, imgs = cfg
    tiles = grid_h * grid_w
    lanes = tiles * imgs
    param_refs = refs[0:12]
    out_ref = refs[12]
    (xs, send_in, recv_in, send_out, t0, t1, t2, t3, t4, t5, *rest) = refs[13:]
    param_bufs = rest[0:12]
    (affine, xp, acc_a, y1, z1, y2, z2, y3, s_ref,
     row_sem, load_sem, param_sem, in_send, in_recv, in_own, out_send, out_recv, out_own) = rest[12:]
    w_refs, v_refs = param_bufs[0:6], param_bufs[6:12]
    t_refs = (t0, t1, t2, t3, t4, t5)
    half = th // 2
    width0 = tw * c0
    unit0 = 4 * c0

    my_w, my_h = lax.axis_index("w"), lax.axis_index("h")
    me = my_w * grid_h + my_h
    others = tiles - 1

    def peer(n):
        offset = n + 1
        pw = lax.rem(my_w + offset // grid_h, grid_w)
        ph = lax.rem(my_h + lax.rem(offset, grid_h), grid_h)
        return pw, ph, pw * grid_h + ph

    def loop(lower, upper, body):
        def step_body(n, carry):
            body(n)
            return carry
        lax.fori_loop(lower, upper, step_body, 0)

    def load(k):
        return pltpu.make_async_copy(x_ref.at[:, :, :, pl.ds(pl.multiple_of(k * lanes, lanes), lanes)], xs.at[k], load_sem.at[k])

    barrier = pltpu.get_barrier_semaphore()
    in_column = [dw * grid_h for dw in range(1, grid_w)]
    near = in_column + list(range(1, grid_h))

    def greet(semaphore, offset):
        pw, ph, _ = peer(offset - 1)
        pl.semaphore_signal(semaphore, inc=1, device_id={"w": pw, "h": ph}, device_id_type=MESH)

    for offset in near:
        greet(barrier, offset)
    loop(0, CHUNKS, lambda k: load(k).start())
    params = [pltpu.make_async_copy(param_refs[n], param_bufs[n], param_sem.at[n]) for n in range(12)]
    for param in params:
        param.start()
    pl.semaphore_wait(barrier, len(near))
    for offset in in_column:
        greet(row_sem, offset)

    def iota(shape, dim):
        return lax.broadcasted_iota(jnp.int32, shape, dim)

    both = 2 * lanes
    o, i = iota((both, both), 0), iota((both, both), 1)
    o_tile, o_half, o_img = o // (2 * imgs), (o // imgs) % 2, o % imgs
    pair = jnp.where(i == o_half * lanes + o_tile * imgs + o_img, 1.0, 0.0).astype(BF16)

    def pack(k):
        load(k).wait()
        for r in range(half):
            cat = jnp.concatenate([xs[k, r].reshape(width0, lanes), xs[k, r + half].reshape(width0, lanes)], axis=1)
            res = lax.dot_general(pair, cat, (((1,), (1,)), ((), ())), preferred_element_type=F32)
            send_in[k, :, :, r * width0:(r + 1) * width0] = res.reshape(tiles, 2 * imgs, width0).astype(BF16)

    def copy_in(k, n):
        pw, ph, p = peer(n)
        return pltpu.make_async_remote_copy(
            src_ref=send_in.at[k, p], dst_ref=recv_in.at[k, me], send_sem=in_send.at[k, n], recv_sem=in_recv.at[k, n],
            device_id={"w": pw, "h": ph}, device_id_type=MESH)

    def own_in(k):
        return pltpu.make_async_copy(send_in.at[k, me], recv_in.at[k, me], in_own.at[k])

    def copy_out(k, n):
        pw, ph, p = peer(n)
        return pltpu.make_async_remote_copy(
            src_ref=send_out.at[k, p], dst_ref=out_ref.at[k, me], send_sem=out_send.at[k, n], recv_sem=out_recv.at[k, n],
            device_id={"w": pw, "h": ph}, device_id_type=MESH)

    def own_out(k):
        return pltpu.make_async_copy(send_out.at[k, me], out_ref.at[k, me], out_own.at[k])

    def start(k, copy, own, seed=SEED):
        for offset in send_order(grid_w, grid_h, seed):
            copy(k, offset - 1).start()
        own(k).start()

    def wait(k, copy, own):
        loop(0, others, lambda n: copy(k, n).wait())
        own(k).wait()

    pack(0)
    pl.semaphore_wait(row_sem, len(in_column))
    start(0, copy_in, own_in)

    def pack_body(k):
        pack(k)
        pl.when(k < CHUNKS - 1)(lambda: start(k, copy_in, own_in))

    loop(1, CHUNKS, pack_body)

    for param in params:
        param.wait()
    for layer, (stride, bh, bw) in enumerate(BLOCKS):
        w_ref = w_refs[layer]
        ci, co = w_ref.shape[2], w_ref.shape[3]
        rows, cols = patch_shape(stride, bh, bw, layer == 0)
        off = 3 if layer == 0 else 0
        bands = [jnp.concatenate([w_ref[dy, dx].astype(F32) for dx in range(3)], axis=0).T for dy in range(3)]
        for bi in range(bh):
            for bj in range(bw):
                parts, at = [], 0
                for dy in range(3):
                    begin = ((stride * bi + dy) * cols + off + stride * bj) * ci
                    if begin > at:
                        parts.append(jnp.zeros((co, begin - at), F32))
                    parts.append(bands[dy])
                    at = begin + 3 * ci
                if rows * cols * ci > at:
                    parts.append(jnp.zeros((co, rows * cols * ci - at), F32))
                t_refs[layer][(bi * bw + bj) * co:(bi * bw + bj + 1) * co] = jnp.concatenate(parts, axis=1).astype(BF16)
        for q in range(3):
            affine[layer, q, 0:co] = jnp.broadcast_to(v_refs[layer][q:q + 1], (lanes, co)).T

    src_l, dst_l = iota((lanes, lanes), 0), iota((lanes, lanes), 1)
    same_image = jnp.where(src_l % imgs == dst_l % imgs, 1.0, 0.0).astype(BF16)
    lane = iota((16, lanes), 1)
    lane_h, lane_w = (lane // imgs) % grid_h, lane // (imgs * grid_h)

    def mask(dh, dw):
        h, w = lane_h + dh, lane_w + dw
        inside = (h >= 0) & (h < grid_h) & (w >= 0) & (w < grid_w)
        return jnp.where(inside, 1.0, 0.0).astype(BF16)

    masks = {(dh, dw): mask(dh, dw) for dh in (-1, 0, 1) for dw in (-1, 0, 1) if (dh, dw) != (0, 0)}

    def take(value, dh, dw):
        shift = (-(dh + dw * grid_h) * imgs) % lanes
        moved = pltpu.roll(value, shift, 1).reshape(-1, 16, lanes)
        return (moved * masks[(dh, dw)][None]).reshape(value.shape)

    def halos(buf, rows, cols, unit, both_sides):
        sides = (-1, 0, 1) if both_sides else (-1, 0)
        for dh in sides:
            for dw in sides:
                if (dh, dw) == (0, 0):
                    continue
                src_r = {-1: (rows, rows + 1), 0: (1, rows + 1), 1: (1, 2)}[dh]
                dst_r = {-1: 0, 0: 1, 1: rows + 1}[dh]
                src_c = {-1: (cols, cols + 1), 0: (1, cols + 1), 1: (1, 2)}[dw]
                dst_c = {-1: 0, 0: 1, 1: cols + 1}[dw]
                span = (src_c[1] - src_c[0]) * unit
                for n in range(src_r[1] - src_r[0]):
                    value = buf[src_r[0] + n, src_c[0] * unit:src_c[1] * unit]
                    buf[dst_r + n, dst_c * unit:dst_c * unit + span] = take(value, dh, dw)

    def conv(buf, w_ref, stride, bh, bw, ci, co, out_h, out_w, first):
        rows, cols = patch_shape(stride, bh, bw, first)
        s_ref[:, 0:co] = jnp.zeros((2, co, lanes), F32)
        far = out_h // 2

        def row_body(n, carry):
            for j in range(out_w // bw):
                start = j * bw * stride * ci
                patches = []
                for base in (n * bh, n * bh + far):
                    patches.append(jnp.concatenate([buf[base * stride + r, start:start + cols * ci] for r in range(rows)], axis=0))
                res = jnp.dot(w_ref[...], jnp.concatenate(patches, axis=1), preferred_element_type=F32)
                parts = [res[p * co:(p + 1) * co, q * lanes:(q + 1) * lanes] for p in range(bh * bw) for q in range(2)]
                s_ref[0, 0:co] += functools.reduce(jnp.add, parts)
                s_ref[1, 0:co] += functools.reduce(jnp.add, [p * p for p in parts])
                for b in range(bh):
                    for q in range(2):
                        acc_a[n * bh + b + q * far, j * bw * co:(j + 1) * bw * co] = res[b * bw * co:(b + 1) * bw * co, q * lanes:(q + 1) * lanes]
            return carry

        lax.fori_loop(0, far // bh, row_body, 0)

    def group_sum(x, co):
        per = co // NORM_GROUPS
        span = max(per, 8)
        y = x.reshape(co // span, span, lanes)
        if per >= 8:
            return jnp.broadcast_to(jnp.sum(y, axis=1, keepdims=True), y.shape).reshape(co, lanes)
        row = iota((1, span, lanes), 1) // per
        res = jnp.zeros_like(y)
        for g in range(span // per):
            part = jnp.sum(jnp.where(row == g, y, 0.0), axis=1, keepdims=True)
            res = jnp.where(row == g, part, res)
        return res.reshape(co, lanes)

    def stats(layer, co, pixels):
        bias, gain, shift = affine[layer, 0, 0:co], affine[layer, 1, 0:co], affine[layer, 2, 0:co]
        s1, s2 = s_ref[0, 0:co], s_ref[1, 0:co]
        with_bias = pixels * bias
        part = jnp.concatenate([group_sum(s1 + with_bias, co), group_sum(s2 + bias * (2.0 * s1 + with_bias), co)], axis=0)
        p0 = part.astype(BF16)
        rest = part - p0.astype(F32)
        p1 = rest.astype(BF16)
        p2 = (rest - p1.astype(F32)).astype(BF16)
        tot = jnp.dot(jnp.concatenate([p0, p1, p2], axis=0), same_image, preferred_element_type=F32)
        tot = (tot[0:2 * co] + tot[2 * co:4 * co] + tot[4 * co:6 * co]) * (1.0 / (pixels * tiles * (co // NORM_GROUPS)))
        m = tot[0:co]
        q = jnp.maximum(tot[co:2 * co] - m * m, 0.0)
        scale = lax.rsqrt(q + NORM_EPS) * gain
        return scale, shift + (bias - m) * scale

    def normalise(scale, offset, co, out_h, out_w, dst_buf):
        def row_body(r, carry):
            for j in range(out_w):
                val = acc_a[r, j * co:(j + 1) * co]
                dst_buf[r + 1, (j + 1) * co:(j + 2) * co] = jnp.maximum(val * scale + offset, 0.0).astype(BF16)
            return carry

        lax.fori_loop(0, out_h, row_body, 0)

    bufs = (xp, y1, z1, y2, z2, y3)

    def chunk(k):
        wait(k, copy_in, own_in)
        pl.when(k == 0)(lambda: start(CHUNKS - 1, copy_in, own_in))
        for r in range(half):
            block = recv_in[k, :, :, r * width0:(r + 1) * width0].astype(F32).reshape(both, width0)
            res = jnp.dot(block.T.astype(BF16), pair, preferred_element_type=F32).astype(BF16)
            xp[r + 1, unit0:unit0 + width0] = res[:, 0:lanes]
            xp[r + 1 + half, unit0:unit0 + width0] = res[:, lanes:both]
        xp[0, unit0:unit0 + width0] = take(xp[th, unit0:unit0 + width0], -1, 0)
        xp[0, 0:unit0] = take(xp[th, width0:width0 + unit0], -1, -1)
        for r in range(1, th + 1):
            xp[r, 0:unit0] = take(xp[r, width0:width0 + unit0], 0, -1)

        h, w, ci = th, tw, c0
        for layer in range(6):
            stride, bh, bw = BLOCKS[layer]
            co = widths[layer // 2]
            h, w = h // stride, w // stride
            conv(bufs[layer], t_refs[layer], stride, bh, bw, ci, co, h, w, layer == 0)
            scale, offset = stats(layer, co, float(h * w))
            ci = co
            if layer < 5:
                normalise(scale, offset, co, h, w, bufs[layer + 1])
                halos(bufs[layer + 1], h, w, co, layer % 2 == 0)

        def finish(p):
            r, j = p // w, p % w
            return jnp.maximum(acc_a[r, j * ci:(j + 1) * ci] * scale + offset, 0.0).astype(BF16)

        for p in range(h * w // 2):
            cat = jnp.concatenate([finish(p), finish(p + h * w // 2)], axis=1)
            res = lax.dot_general(pair, cat, (((1,), (1,)), ((), ())), preferred_element_type=F32)
            send_out[k, :, p] = res.reshape(tiles, 2 * imgs, ci).astype(BF16)
        start(k, copy_out, own_out, OUT_SEED)

    loop(0, CHUNKS, chunk)
    loop(0, CHUNKS, lambda k: wait(k, copy_out, own_out))


def encode(cfg, x, kernels, affines):
    th, tw, c0, widths, grid_h, grid_w, imgs = cfg
    tiles = grid_h * grid_w
    lanes = tiles * imgs
    c1, c2, c3 = widths
    h1, w1, h2, w2, h3, w3 = th // 2, tw // 2, th // 4, tw // 4, th // 8, tw // 8
    tables = []
    for layer, (stride, bh, bw) in enumerate(BLOCKS):
        rows, cols = patch_shape(stride, bh, bw, layer == 0)
        tables.append(pltpu.VMEM((bh * bw * kernels[layer].shape[3], rows * cols * kernels[layer].shape[2]), BF16))
    dma = pltpu.SemaphoreType.DMA
    return pl.pallas_call(
        functools.partial(encoder_kernel, cfg),
        out_shape=jax.ShapeDtypeStruct((CHUNKS, tiles, h3 * w3 // 2, 2 * imgs, c3), BF16),
        in_specs=[pl.BlockSpec(memory_space=pltpu.HBM)] * 13,
        out_specs=pl.BlockSpec(memory_space=pl.ANY),
        scratch_shapes=[
            pltpu.VMEM((CHUNKS, th, tw, c0, lanes), BF16),
            pltpu.VMEM((CHUNKS, tiles, 2 * imgs, th * tw * c0 // 2), BF16),
            pltpu.VMEM((CHUNKS, tiles, 2 * imgs, th * tw * c0 // 2), BF16),
            pltpu.VMEM((CHUNKS, tiles, h3 * w3 // 2, 2 * imgs, c3), BF16),
            *tables,
            *[pltpu.VMEM(p.shape, p.dtype) for p in (*kernels, *affines)],
            pltpu.VMEM((6, 3, c3, lanes), F32),
            pltpu.VMEM((th + 1, (tw + 4) * c0, lanes), BF16),
            pltpu.VMEM((h1, w1 * c1, lanes), F32),
            pltpu.VMEM((h1 + 2, (w1 + 2) * c1, lanes), BF16),
            pltpu.VMEM((h1 + 1, (w1 + 1) * c1, lanes), BF16),
            pltpu.VMEM((h2 + 2, (w2 + 2) * c2, lanes), BF16),
            pltpu.VMEM((h2 + 1, (w2 + 1) * c2, lanes), BF16),
            pltpu.VMEM((h3 + 2, (w3 + 2) * c3, lanes), BF16),
            pltpu.VMEM((2, c3, lanes), F32),
            pltpu.SemaphoreType.REGULAR, dma((CHUNKS,)), dma((12,)),
            dma((CHUNKS, tiles - 1)), dma((CHUNKS, tiles - 1)), dma((CHUNKS,)),
            dma((CHUNKS, tiles - 1)), dma((CHUNKS, tiles - 1)), dma((CHUNKS,)),
        ],
        compiler_params=pltpu.CompilerParams(vmem_limit_bytes=40 * 1024 * 1024, collective_id=0, has_side_effects=True),
    )(*[pltpu.with_memory_space_constraint(p, pltpu.HBM) for p in (x, *kernels, *affines)])


def solution(mesh):
    grid_h = mesh.shape["h"]
    grid_w = mesh.shape["w"]
    tiles = grid_h * grid_w
    act_spec = P("batch", "h", "w")

    def local_forward(tile, *params):
        count, th, tw, c0 = tile.shape
        kernels, affines = params[0::2], params[1::2]
        widths = tuple(kernels[2 * s].shape[3] for s in range(3))
        cfg = (th, tw, c0, widths, grid_h, grid_w, count // tiles // CHUNKS)
        res = encode(cfg, tile.transpose(1, 2, 3, 0), kernels, affines)
        imgs = count // tiles // CHUNKS
        res = res.reshape(CHUNKS, tiles, -1, 2, imgs, widths[2])
        return res.transpose(0, 1, 4, 3, 2, 5).reshape(count, th // 8, tw // 8, widths[2])

    return jax.shard_map(local_forward, mesh=mesh, in_specs=(act_spec,) + (P(),) * 12, out_specs=act_spec, check_vma=False)
```

```python
import functools
import random

import jax
import jax.numpy as jnp
from jax import lax
from jax.experimental import pallas as pl
from jax.experimental.pallas import tpu as pltpu
from jax.sharding import PartitionSpec as P

NORM_GROUPS = 8
NORM_EPS = 1e-5
CHUNKS = 4
SEED = 22
OUT_SEED = 3
BLOCKS = ((2, 1, 8), (1, 2, 4), (2, 1, 2), (1, 2, 2), (2, 1, 2), (1, 1, 2))
MESH = pl.DeviceIdType.MESH
BF16, F32 = jnp.bfloat16, jnp.float32


def send_order(grid_w, grid_h, seed=SEED):
    order = list(range(1, grid_w * grid_h))
    random.Random(seed).shuffle(order)
    return order


def patch_shape(stride, bh, bw, first):
    rows = (bh - 1) * stride + 3
    cols = (bw - 1) * stride + 3
    if first:
        cols = bw * stride + 4
    return rows, cols


def encoder_kernel(cfg, x_ref, *refs):
    th, tw, c0, widths, grid_h, grid_w, imgs = cfg
    tiles = grid_h * grid_w
    lanes = tiles * imgs
    param_refs = refs[0:12]
    out_ref = refs[12]
    (xs, send_in, recv_in, send_out, t0, t1, t2, t3, t4, t5, *rest) = refs[13:]
    param_bufs = rest[0:12]
    (affine, xp, acc_a, y1, z1, y2, z2, y3, s_ref,
     row_sem, load_sem, param_sem, in_send, in_recv, in_own, out_send, out_recv, out_own) = rest[12:]
    w_refs, v_refs = param_bufs[0:6], param_bufs[6:12]
    t_refs = (t0, t1, t2, t3, t4, t5)
    half = th // 2
    width0 = tw * c0
    unit0 = 4 * c0

    my_w, my_h = lax.axis_index("w"), lax.axis_index("h")
    me = my_w * grid_h + my_h
    others = tiles - 1

    def peer(n):
        offset = n + 1
        pw = lax.rem(my_w + offset // grid_h, grid_w)
        ph = lax.rem(my_h + lax.rem(offset, grid_h), grid_h)
        return pw, ph, pw * grid_h + ph

    def loop(lower, upper, body):
        def step_body(n, carry):
            body(n)
            return carry
        lax.fori_loop(lower, upper, step_body, 0)

    def load(k):
        return pltpu.make_async_copy(x_ref.at[:, :, :, pl.ds(pl.multiple_of(k * lanes, lanes), lanes)], xs.at[k], load_sem.at[k])

    barrier = pltpu.get_barrier_semaphore()
    in_column = [dw * grid_h for dw in range(1, grid_w)]
    near = in_column + list(range(1, grid_h))

    def greet(semaphore, offset):
        pw, ph, _ = peer(offset - 1)
        pl.semaphore_signal(semaphore, inc=1, device_id={"w": pw, "h": ph}, device_id_type=MESH)

    for offset in near:
        greet(barrier, offset)
    loop(0, CHUNKS, lambda k: load(k).start())
    params = [pltpu.make_async_copy(param_refs[n], param_bufs[n], param_sem.at[n]) for n in range(12)]
    for param in params:
        param.start()
    pl.semaphore_wait(barrier, len(near))
    for offset in in_column:
        greet(row_sem, offset)

    def iota(shape, dim):
        return lax.broadcasted_iota(jnp.int32, shape, dim)

    both = 2 * lanes
    o, i = iota((both, both), 0), iota((both, both), 1)
    o_tile, o_half, o_img = o // (2 * imgs), (o // imgs) % 2, o % imgs
    pair = jnp.where(i == o_half * lanes + o_tile * imgs + o_img, 1.0, 0.0).astype(BF16)

    def pack(k):
        load(k).wait()
        for r in range(half):
            cat = jnp.concatenate([xs[k, r].reshape(width0, lanes), xs[k, r + half].reshape(width0, lanes)], axis=1)
            res = lax.dot_general(pair, cat, (((1,), (1,)), ((), ())), preferred_element_type=F32)
            send_in[k, :, :, r * width0:(r + 1) * width0] = res.reshape(tiles, 2 * imgs, width0).astype(BF16)

    def copy_in(k, n):
        pw, ph, p = peer(n)
        return pltpu.make_async_remote_copy(
            src_ref=send_in.at[k, p], dst_ref=recv_in.at[k, me], send_sem=in_send.at[k, n], recv_sem=in_recv.at[k, n],
            device_id={"w": pw, "h": ph}, device_id_type=MESH)

    def own_in(k):
        return pltpu.make_async_copy(send_in.at[k, me], recv_in.at[k, me], in_own.at[k])

    def copy_out(k, n):
        pw, ph, p = peer(n)
        return pltpu.make_async_remote_copy(
            src_ref=send_out.at[k, p], dst_ref=out_ref.at[k, me], send_sem=out_send.at[k, n], recv_sem=out_recv.at[k, n],
            device_id={"w": pw, "h": ph}, device_id_type=MESH)

    def own_out(k):
        return pltpu.make_async_copy(send_out.at[k, me], out_ref.at[k, me], out_own.at[k])

    def start(k, copy, own, seed=SEED):
        for offset in send_order(grid_w, grid_h, seed):
            copy(k, offset - 1).start()
        own(k).start()

    def wait(k, copy, own):
        loop(0, others, lambda n: copy(k, n).wait())
        own(k).wait()

    pack(0)
    pl.semaphore_wait(row_sem, len(in_column))
    start(0, copy_in, own_in)

    def pack_body(k):
        pack(k)
        pl.when(k < CHUNKS - 1)(lambda: start(k, copy_in, own_in))

    loop(1, CHUNKS, pack_body)

    for param in params:
        param.wait()
    for layer, (stride, bh, bw) in enumerate(BLOCKS):
        w_ref = w_refs[layer]
        ci, co = w_ref.shape[2], w_ref.shape[3]
        rows, cols = patch_shape(stride, bh, bw, layer == 0)
        off = 3 if layer == 0 else 0
        bands = [jnp.concatenate([w_ref[dy, dx].astype(F32) for dx in range(3)], axis=0).T for dy in range(3)]
        for bi in range(bh):
            for bj in range(bw):
                parts, at = [], 0
                for dy in range(3):
                    begin = ((stride * bi + dy) * cols + off + stride * bj) * ci
                    if begin > at:
                        parts.append(jnp.zeros((co, begin - at), F32))
                    parts.append(bands[dy])
                    at = begin + 3 * ci
                if rows * cols * ci > at:
                    parts.append(jnp.zeros((co, rows * cols * ci - at), F32))
                t_refs[layer][(bi * bw + bj) * co:(bi * bw + bj + 1) * co] = jnp.concatenate(parts, axis=1).astype(BF16)
        for q in range(3):
            affine[layer, q, 0:co] = jnp.broadcast_to(v_refs[layer][q:q + 1], (lanes, co)).T

    src_l, dst_l = iota((lanes, lanes), 0), iota((lanes, lanes), 1)
    same_image = jnp.where(src_l % imgs == dst_l % imgs, 1.0, 0.0).astype(BF16)
    lane = iota((16, lanes), 1)
    lane_h, lane_w = (lane // imgs) % grid_h, lane // (imgs * grid_h)

    def mask(dh, dw):
        h, w = lane_h + dh, lane_w + dw
        inside = (h >= 0) & (h < grid_h) & (w >= 0) & (w < grid_w)
        return jnp.where(inside, 1.0, 0.0).astype(BF16)

    masks = {(dh, dw): mask(dh, dw) for dh in (-1, 0, 1) for dw in (-1, 0, 1) if (dh, dw) != (0, 0)}

    def take(value, dh, dw):
        shift = (-(dh + dw * grid_h) * imgs) % lanes
        moved = pltpu.roll(value, shift, 1).reshape(-1, 16, lanes)
        return (moved * masks[(dh, dw)][None]).reshape(value.shape)

    def halos(buf, rows, cols, unit, both_sides):
        sides = (-1, 0, 1) if both_sides else (-1, 0)
        for dh in sides:
            for dw in sides:
                if (dh, dw) == (0, 0):
                    continue
                src_r = {-1: (rows, rows + 1), 0: (1, rows + 1), 1: (1, 2)}[dh]
                dst_r = {-1: 0, 0: 1, 1: rows + 1}[dh]
                src_c = {-1: (cols, cols + 1), 0: (1, cols + 1), 1: (1, 2)}[dw]
                dst_c = {-1: 0, 0: 1, 1: cols + 1}[dw]
                span = (src_c[1] - src_c[0]) * unit
                for n in range(src_r[1] - src_r[0]):
                    value = buf[src_r[0] + n, src_c[0] * unit:src_c[1] * unit]
                    buf[dst_r + n, dst_c * unit:dst_c * unit + span] = take(value, dh, dw)

    def conv(buf, w_ref, stride, bh, bw, ci, co, out_h, out_w, first):
        rows, cols = patch_shape(stride, bh, bw, first)
        s_ref[:, 0:co] = jnp.zeros((2, co, lanes), F32)
        far = out_h // 2

        def row_body(n, carry):
            for j in range(out_w // bw):
                start = j * bw * stride * ci
                patches = []
                for base in (n * bh, n * bh + far):
                    patches.append(jnp.concatenate([buf[base * stride + r, start:start + cols * ci] for r in range(rows)], axis=0))
                res = jnp.dot(w_ref[...], jnp.concatenate(patches, axis=1), preferred_element_type=F32)
                parts = [res[p * co:(p + 1) * co, q * lanes:(q + 1) * lanes] for p in range(bh * bw) for q in range(2)]
                s_ref[0, 0:co] += functools.reduce(jnp.add, parts)
                s_ref[1, 0:co] += functools.reduce(jnp.add, [p * p for p in parts])
                for b in range(bh):
                    for q in range(2):
                        acc_a[n * bh + b + q * far, j * bw * co:(j + 1) * bw * co] = res[b * bw * co:(b + 1) * bw * co, q * lanes:(q + 1) * lanes]
            return carry

        lax.fori_loop(0, far // bh, row_body, 0)

    def group_sum(x, co):
        per = co // NORM_GROUPS
        span = max(per, 8)
        y = x.reshape(co // span, span, lanes)
        if per >= 8:
            return jnp.broadcast_to(jnp.sum(y, axis=1, keepdims=True), y.shape).reshape(co, lanes)
        row = iota((1, span, lanes), 1) // per
        res = jnp.zeros_like(y)
        for g in range(span // per):
            part = jnp.sum(jnp.where(row == g, y, 0.0), axis=1, keepdims=True)
            res = jnp.where(row == g, part, res)
        return res.reshape(co, lanes)

    def stats(layer, co, pixels):
        bias, gain, shift = affine[layer, 0, 0:co], affine[layer, 1, 0:co], affine[layer, 2, 0:co]
        s1, s2 = s_ref[0, 0:co], s_ref[1, 0:co]
        with_bias = pixels * bias
        part = jnp.concatenate([group_sum(s1 + with_bias, co), group_sum(s2 + bias * (2.0 * s1 + with_bias), co)], axis=0)
        p0 = part.astype(BF16)
        rest = part - p0.astype(F32)
        p1 = rest.astype(BF16)
        p2 = (rest - p1.astype(F32)).astype(BF16)
        tot = jnp.dot(jnp.concatenate([p0, p1, p2], axis=0), same_image, preferred_element_type=F32)
        tot = (tot[0:2 * co] + tot[2 * co:4 * co] + tot[4 * co:6 * co]) * (1.0 / (pixels * tiles * (co // NORM_GROUPS)))
        m = tot[0:co]
        q = jnp.maximum(tot[co:2 * co] - m * m, 0.0)
        scale = lax.rsqrt(q + NORM_EPS) * gain
        return scale, shift + (bias - m) * scale

    def normalise(scale, offset, co, out_h, out_w, dst_buf):
        def row_body(r, carry):
            for j in range(out_w):
                val = acc_a[r, j * co:(j + 1) * co]
                dst_buf[r + 1, (j + 1) * co:(j + 2) * co] = jnp.maximum(val * scale + offset, 0.0).astype(BF16)
            return carry

        lax.fori_loop(0, out_h, row_body, 0)

    bufs = (xp, y1, z1, y2, z2, y3)

    def chunk(k):
        wait(k, copy_in, own_in)
        pl.when(k == 0)(lambda: start(CHUNKS - 1, copy_in, own_in))
        for r in range(half):
            block = recv_in[k, :, :, r * width0:(r + 1) * width0].astype(F32).reshape(both, width0)
            res = jnp.dot(block.T.astype(BF16), pair, preferred_element_type=F32).astype(BF16)
            xp[r + 1, unit0:unit0 + width0] = res[:, 0:lanes]
            xp[r + 1 + half, unit0:unit0 + width0] = res[:, lanes:both]
        xp[0, unit0:unit0 + width0] = take(xp[th, unit0:unit0 + width0], -1, 0)
        xp[0, 0:unit0] = take(xp[th, width0:width0 + unit0], -1, -1)
        for r in range(1, th + 1):
            xp[r, 0:unit0] = take(xp[r, width0:width0 + unit0], 0, -1)

        h, w, ci = th, tw, c0
        for layer in range(6):
            stride, bh, bw = BLOCKS[layer]
            co = widths[layer // 2]
            h, w = h // stride, w // stride
            conv(bufs[layer], t_refs[layer], stride, bh, bw, ci, co, h, w, layer == 0)
            scale, offset = stats(layer, co, float(h * w))
            ci = co
            if layer < 5:
                normalise(scale, offset, co, h, w, bufs[layer + 1])
                halos(bufs[layer + 1], h, w, co, layer % 2 == 0)

        def finish(p):
            r, j = p // w, p % w
            return jnp.maximum(acc_a[r, j * ci:(j + 1) * ci] * scale + offset, 0.0).astype(BF16)

        for p in range(h * w // 2):
            cat = jnp.concatenate([finish(p), finish(p + h * w // 2)], axis=1)
            res = lax.dot_general(pair, cat, (((1,), (1,)), ((), ())), preferred_element_type=F32)
            send_out[k, :, p] = res.reshape(tiles, 2 * imgs, ci).astype(BF16)
        start(k, copy_out, own_out, OUT_SEED)

    loop(0, CHUNKS, chunk)
    loop(0, CHUNKS, lambda k: wait(k, copy_out, own_out))


def encode(cfg, x, kernels, affines):
    th, tw, c0, widths, grid_h, grid_w, imgs = cfg
    tiles = grid_h * grid_w
    lanes = tiles * imgs
    c1, c2, c3 = widths
    h1, w1, h2, w2, h3, w3 = th // 2, tw // 2, th // 4, tw // 4, th // 8, tw // 8
    tables = []
    for layer, (stride, bh, bw) in enumerate(BLOCKS):
        rows, cols = patch_shape(stride, bh, bw, layer == 0)
        tables.append(pltpu.VMEM((bh * bw * kernels[layer].shape[3], rows * cols * kernels[layer].shape[2]), BF16))
    dma = pltpu.SemaphoreType.DMA
    return pl.pallas_call(
        functools.partial(encoder_kernel, cfg),
        out_shape=jax.ShapeDtypeStruct((CHUNKS, tiles, h3 * w3 // 2, 2 * imgs, c3), BF16),
        in_specs=[pl.BlockSpec(memory_space=pltpu.HBM)] * 13,
        out_specs=pl.BlockSpec(memory_space=pl.ANY),
        scratch_shapes=[
            pltpu.VMEM((CHUNKS, th, tw, c0, lanes), BF16),
            pltpu.VMEM((CHUNKS, tiles, 2 * imgs, th * tw * c0 // 2), BF16),
            pltpu.VMEM((CHUNKS, tiles, 2 * imgs, th * tw * c0 // 2), BF16),
            pltpu.VMEM((CHUNKS, tiles, h3 * w3 // 2, 2 * imgs, c3), BF16),
            *tables,
            *[pltpu.VMEM(p.shape, p.dtype) for p in (*kernels, *affines)],
            pltpu.VMEM((6, 3, c3, lanes), F32),
            pltpu.VMEM((th + 1, (tw + 4) * c0, lanes), BF16),
            pltpu.VMEM((h1, w1 * c1, lanes), F32),
            pltpu.VMEM((h1 + 2, (w1 + 2) * c1, lanes), BF16),
            pltpu.VMEM((h1 + 1, (w1 + 1) * c1, lanes), BF16),
            pltpu.VMEM((h2 + 2, (w2 + 2) * c2, lanes), BF16),
            pltpu.VMEM((h2 + 1, (w2 + 1) * c2, lanes), BF16),
            pltpu.VMEM((h3 + 2, (w3 + 2) * c3, lanes), BF16),
            pltpu.VMEM((2, c3, lanes), F32),
            pltpu.SemaphoreType.REGULAR, dma((CHUNKS,)), dma((12,)),
            dma((CHUNKS, tiles - 1)), dma((CHUNKS, tiles - 1)), dma((CHUNKS,)),
            dma((CHUNKS, tiles - 1)), dma((CHUNKS, tiles - 1)), dma((CHUNKS,)),
        ],
        compiler_params=pltpu.CompilerParams(vmem_limit_bytes=40 * 1024 * 1024, collective_id=0, has_side_effects=True),
    )(*[pltpu.with_memory_space_constraint(p, pltpu.HBM) for p in (x, *kernels, *affines)])


def solution(mesh):
    grid_h = mesh.shape["h"]
    grid_w = mesh.shape["w"]
    tiles = grid_h * grid_w
    act_spec = P("batch", "h", "w")

    def local_forward(tile, *params):
        count, th, tw, c0 = tile.shape
        kernels, affines = params[0::2], params[1::2]
        widths = tuple(kernels[2 * s].shape[3] for s in range(3))
        cfg = (th, tw, c0, widths, grid_h, grid_w, count // tiles // CHUNKS)
        res = encode(cfg, tile.transpose(1, 2, 3, 0), kernels, affines)
        imgs = count // tiles // CHUNKS
        res = res.reshape(CHUNKS, tiles, -1, 2, imgs, widths[2])
        return res.transpose(0, 1, 4, 3, 2, 5).reshape(count, th // 8, tw // 8, widths[2])

    return jax.shard_map(local_forward, mesh=mesh, in_specs=(act_spec,) + (P(),) * 12, out_specs=act_spec, check_vma=False)
```
